256 devices in a mesh: rows: 64 (over y, z, core), rep: 4 (over x).
Axes of the slice: x: 4, y: 4, z: 8, core: 2. Of those that a mesh axis runs over, the one named last changes fastest.
Arguments:
- binned: int32 [65536, 1024], P('rows', 'rep'), may hold values from 0 to 127
- gradients: bfloat16 [65536], P('rows'), may hold values from -3 to 3
- hessians: bfloat16 [65536], P('rows'), may hold values from 0.019897461 to 0.25
- parents: int32 [65536], P('rows'), may hold values from 0 to 15
- split_feature: int32 [16], replicated, may hold values from 0 to 1023
- split_bin: int32 [16], replicated, may hold values from 32 to 95
- elected: int32 [32, 512], P(None, 'rep'), may hold values from 0 to 255
Outputs:
- new_nodes: int32 [65536], P('rows')
- best_gain: float32 [32, 4, 128], P(None, 'rep', 'rows')
- node_best: float32 [32], replicated
The draws below stay inside these ranges and needn't reach their ends.
All inputs are finite; a program needn't handle non-finite values.
Results may differ from the reference program's by a relative error of at most 0.0003.
Values sent between devices are 32-bit elements; how exact they have to be, the bound alone decides.
A program may use at most 64 MiB of HBM per device.

```python
import math
import jax
import jax.numpy as jnp

F = 1024
BINS = 128
ELECT = 512
NODES = 32
PARENTS = 16
ROWS = 65536
N_REP = 4


def plant(result, key, least, largest):
    longest = result.shape.index(max(result.shape))
    spots = []
    for shift in (0, 1):
        where = [jax.random.randint(jax.random.fold_in(key, axis), (), 0, length) for axis, length in enumerate(result.shape)]
        where[longest] = (where[longest] + shift) % result.shape[longest]
        spots.append(tuple(where))
    return result.at[spots[0]].set(least).at[spots[1]].set(largest)


def level_of(rng, shape, cuts, least, high):
    def one(axis_at, blocks):
        steps = jax.random.uniform(jax.random.fold_in(jax.random.fold_in(rng, 6), axis_at), (blocks,), jnp.float32, least / len(cuts), high / len(cuts))
        return jnp.repeat(jnp.exp(steps), shape[axis_at] // blocks).reshape((-1,) + (1,) * (len(shape) - axis_at - 1))

    level = one(*cuts[0])
    for cut in cuts[1:]:
        level = level * one(*cut)
    return level


def centred(own_key, extent, deviation, bound, pieces=(), kind=jnp.bfloat16):
    loudness = level_of(own_key, extent, pieces, -0.22, 0.18) if pieces else 1.0
    drawn = jax.random.normal(own_key, extent, jnp.float32) * deviation * loudness
    return jnp.minimum(jnp.maximum(drawn, -bound), bound).astype(kind)


def setup_inputs(seed: int = 0) -> dict:
    seeds = jax.random.split(jax.random.key(seed), 8)
    return {
        "binned": plant(jax.random.randint(seeds[0], (ROWS, F), 0, BINS), jax.random.fold_in(seeds[0], 1), 0, BINS - 1).astype(jnp.int32),
        "gradients": centred(seeds[1], (ROWS,), 0.5, 3.0, ((0, 64),)),
        "hessians": jnp.clip(jnp.exp(math.log(0.25) - 2.5308688 * jax.random.uniform(seeds[2], (ROWS,), jnp.float32) ** level_of(seeds[2], (ROWS,), ((0, 64),), -0.2, 0.2)), 0.019897461, 0.25).astype(jnp.bfloat16),
        "parents": plant(jax.random.randint(seeds[3], (ROWS,), 0, PARENTS), jax.random.fold_in(seeds[3], 1), 0, PARENTS - 1).astype(jnp.int32),
        "split_feature": plant(jax.random.randint(seeds[4], (PARENTS,), 0, F), jax.random.fold_in(seeds[4], 1), 0, F - 1).astype(jnp.int32),
        "split_bin": plant(jax.random.randint(seeds[5], (PARENTS,), BINS // 4, 3 * BINS // 4), jax.random.fold_in(seeds[5], 1), BINS // 4, (3 * BINS // 4) - 1).astype(jnp.int32),
        "elected": plant(jax.random.randint(seeds[6], (NODES, ELECT), 0, F // N_REP), jax.random.fold_in(seeds[6], 1), 0, (F // N_REP) - 1).astype(jnp.int32),
    }


l2_penalty = 1.0


def reference(binned, gradients, hessians, parents, split_feature, split_bin, elected):
    row_feature = split_feature[parents]
    row_value = jnp.take_along_axis(binned, row_feature[:, None], axis=1)[:, 0]
    side_bits = (row_value > split_bin[parents]).astype(jnp.int32)
    new_nodes = (2 * parents + side_bits).astype(jnp.int32)
    slot_ids = jnp.arange(ELECT, dtype=jnp.int32)
    block_start = (slot_ids // (ELECT // N_REP)) * (F // N_REP)
    feature = (elected + block_start[None, :]).astype(jnp.int32)
    row_features = feature[new_nodes]
    row_bins = jnp.take_along_axis(binned, row_features, axis=1)
    segment = (new_nodes[:, None] * ELECT + slot_ids[None, :]) * BINS + row_bins
    segment = segment.astype(jnp.int32).reshape(-1)
    grad_wide = gradients.astype(jnp.float32)
    hess_wide = hessians.astype(jnp.float32)
    count = NODES * ELECT * BINS
    hist_grad = jax.ops.segment_sum(jnp.broadcast_to(grad_wide[:, None], row_bins.shape).reshape(-1), segment, num_segments=count).reshape(NODES, ELECT, BINS)
    hist_hess = jax.ops.segment_sum(jnp.broadcast_to(hess_wide[:, None], row_bins.shape).reshape(-1), segment, num_segments=count).reshape(NODES, ELECT, BINS)
    total_grad = jax.ops.segment_sum(grad_wide, new_nodes, num_segments=NODES)[:, None, None]
    total_hess = jax.ops.segment_sum(hess_wide, new_nodes, num_segments=NODES)[:, None, None]
    left_grad = jnp.cumsum(hist_grad, axis=2)[:, :, :-1]
    left_hess = jnp.cumsum(hist_hess, axis=2)[:, :, :-1]
    split_gain = 0.5 * (left_grad * left_grad / (left_hess + l2_penalty)
                        + (total_grad - left_grad) ** 2 / (total_hess - left_hess + l2_penalty)
                        - total_grad * total_grad / (total_hess + l2_penalty))
    best_slot = jnp.max(split_gain, axis=2)
    best_gain = best_slot.reshape(NODES, N_REP, ELECT // N_REP)
    node_best = jnp.max(best_slot, axis=1)
    return new_nodes, best_gain, node_best
```

```python
import functools

import jax
import jax.numpy as jnp
from jax import lax
from jax.experimental import pallas as pl
from jax.experimental.pallas import tpu as pltpu
from jax.sharding import Mesh
from jax.sharding import PartitionSpec as P

BINS = 128
LANES = 128
ROWS = ("rows_0", "rows_1", "rows_2")
MESH_IDS = pl.DeviceIdType.MESH
f32, bf16, i32 = jnp.float32, jnp.bfloat16, jnp.int32

l2_penalty = 1.0


def iota(shape, dim, dtype=i32):
    out = lax.broadcasted_iota(i32, shape, dim)
    if dtype == bf16:
        return out.astype(f32).astype(bf16)
    return out.astype(dtype)


def remote(src, dst, send, recv, where):
    return pltpu.make_async_remote_copy(
        src_ref=src, dst_ref=dst, send_sem=send, recv_sem=recv, device_id=where, device_id_type=MESH_IDS
    )


def kernel(ny, nz, nx, sc, split_feature, split_bin, meta, elected, binned_hbm,
           nodes_out, best_out, node_best_out,
           binned, side, side_in, outbox, zbox, ybox, acc, acc_in, top, top_z, mid, top_xy,
           load_sem, side_send, side_recv, z_send, z_recv, y_send, y_recv, core_send, core_recv,
           tz_send, tz_recv, txy_send, txy_recv):
    y, z = lax.axis_index("rows_0"), lax.axis_index("rows_1")
    core, x = lax.axis_index("rows_2"), lax.axis_index("rep")
    parent_count = split_feature.shape[0]
    node_count = elected.shape[0]
    width = binned.shape[1]
    chunks = meta.shape[1]

    load = pltpu.make_async_copy(binned_hbm, binned, load_sem)
    load.start()

    def at_x(d):
        return {"rep": lax.rem(x + d, nx)}

    def at_y(d):
        return {"rows_0": lax.rem(y + d, ny)}

    def at_z(d):
        return {"rows_1": lax.rem(z + d, nz)}

    def at_xy(dx, dy):
        return {"rep": lax.rem(x + dx, nx), "rows_0": lax.rem(y + dy, ny)}

    xy = [(dx, dy) for dx in range(nx) for dy in range(ny) if (dx, dy) != (0, 0)]
    peers = [at_z(d) for d in range(1, nz)] + [at_xy(*d) for d in xy] + [{"rows_2": 1 - core}]
    barrier = pltpu.get_barrier_semaphore()
    for peer in peers:
        pl.semaphore_signal(barrier, inc=1, device_id=peer, device_id_type=MESH_IDS)

    load.wait()
    parent_rows = iota((parent_count, LANES), 0)
    want = jnp.zeros((parent_count, width), i32)
    bound = jnp.zeros((parent_count, LANES), i32)
    for p in range(parent_count):
        want = jnp.where(iota((parent_count, width), 0) == p, split_feature[p] - x * width, want)
        bound = jnp.where(parent_rows == p, split_bin[p], bound)
    pick = jnp.where(iota((parent_count, width), 1) == want, jnp.ones((), f32), jnp.zeros((), f32)).astype(bf16)
    owned = (want[:, :LANES] >= 0) & (want[:, :LANES] < width)
    values = lax.dot_general(pick, binned[...].astype(f32).astype(bf16), (((1,), (1,)), ((), ())),
                             preferred_element_type=f32)
    bound = bound.astype(f32)
    for c in range(chunks):
        parent = meta[2, c:c + 1, :]
        hit = (parent_rows.astype(f32) == parent) & owned & (values[:, c * LANES:(c + 1) * LANES] > bound)
        side[c:c + 1, :] = jnp.max(jnp.where(hit, 1.0, 0.0), axis=0, keepdims=True)

    pl.semaphore_wait(barrier, len(peers))
    side_copies = []
    for d in range(1, nx):
        copy = remote(side, side_in.at[d - 1], side_send.at[d - 1], side_recv.at[d - 1], at_x(d))
        copy.start()
        side_copies.append(copy)
    for copy in side_copies:
        copy.wait_recv()
    went = side[...]
    for d in range(1, nx):
        went = went + side_in[d - 1]
    node = 2.0 * meta[2] + went
    nodes_out[...] = node.astype(i32)

    chosen = elected[...].astype(f32).astype(bf16)
    node_rows = iota((node_count, LANES), 0).astype(f32)
    for c in range(chunks):
        hot = jnp.where(node_rows == node[c:c + 1, :], 1.0, 0.0).astype(bf16)
        index = lax.dot_general(hot, chosen, (((0,), (0,)), ((), ())), preferred_element_type=f32).astype(i32)
        inner = index & (LANES - 1)
        picked = None
        for b in range(width // LANES):
            part = jnp.take_along_axis(binned[c * LANES:(c + 1) * LANES, b * LANES:(b + 1) * LANES], inner, axis=1)
            picked = part if b == 0 else jnp.where(index >= b * LANES, part, picked)
        turned = picked.astype(f32).T
        for yy in range(ny):
            for zz in range(nz):
                first = (yy * nz + zz) * sc
                outbox[zz, 3 + yy * sc:3 + (yy + 1) * sc, c, :] = turned[first:first + sc]
    for zz in range(nz):
        outbox[zz, 0:2] = meta[0:2]
        outbox[zz, 2] = node

    def order(i):
        half, odd = (i + 1) // 2, i % 2
        return (odd * half + (1 - odd) * (nz - half)) % nz

    for i in range(1, nz):
        d = order(i)
        remote(outbox.at[lax.rem(z + d, nz)], zbox.at[d], z_send.at[d], z_recv.at[d], at_z(d)).start()
    zbox[0] = outbox[z]

    def forwards(d):
        out = []
        for dy in range(1, ny):
            there = lax.rem(y + dy, ny)
            out.append(remote(zbox.at[d, 0:3], ybox.at[dy - 1, d, 0:3],
                              y_send.at[d, dy - 1, 0], y_recv.at[d, dy - 1], at_y(dy)))
            out.append(remote(zbox.at[d, pl.ds(3 + there * sc, sc)], ybox.at[dy - 1, d, 3:3 + sc],
                              y_send.at[d, dy - 1, 1], y_recv.at[d, dy - 1], at_y(dy)))
        return out

    def add(box, d, shift):
        bin_rows = iota((BINS, LANES), 0, bf16)
        node_of = iota((node_count, LANES), 0, bf16)
        one, zero = jnp.ones((), bf16), jnp.zeros((), bf16)
        grads, hesses = [], []
        for c in range(chunks):
            here = node_of == box[d, 2, c:c + 1, :].astype(bf16)
            grads.append(jnp.where(here, box[d, 0, c:c + 1, :].astype(bf16), zero))
            hesses.append(jnp.where(here, box[d, 1, c:c + 1, :].astype(bf16), zero))
        weights = jnp.concatenate([jnp.concatenate(grads, axis=1), jnp.concatenate(hesses, axis=1)], axis=0)
        hots = []
        for s in range(sc):
            row = [box[d, shift + s, c:c + 1, :].astype(bf16) for c in range(chunks)]
            hots.append(jnp.concatenate([jnp.where(bin_rows == r, one, zero) for r in row], axis=1))
        acc[...] += lax.dot_general(weights, jnp.concatenate(hots, axis=0), (((1,), (1,)), ((), ())),
                                    preferred_element_type=f32)

    def add_all(d):
        add(zbox, d, 3 + y * sc)

        def one(dy, carry):
            pltpu.make_async_copy(ybox.at[dy, d], ybox.at[dy, d], y_recv.at[d, dy]).wait()
            add(ybox.at[dy], d, 3)
            return carry

        lax.fori_loop(0, ny - 1, one, 0)

    acc[...] = jnp.zeros_like(acc)
    for copy in forwards(0):
        copy.start()

    def step(i, carry):
        d = order(i)
        pltpu.make_async_copy(zbox.at[d], zbox.at[d], z_recv.at[d]).wait()
        for copy in forwards(d):
            copy.start()
        add_all(order(i - 1))
        return carry

    lax.fori_loop(1, nz, step, 0)
    add_all(order(nz - 1))

    swap = remote(acc, acc_in, core_send, core_recv, {"rows_2": 1 - core})
    swap.start()
    swap.wait_recv()
    hist = acc[...] + acc_in[...]
    upto = jnp.where(iota((BINS, BINS), 0) <= iota((BINS, BINS), 1), 1.0, 0.0)
    lane = iota((node_count, BINS), 1)
    low = jnp.full((), -3.0e38, f32)
    best = []
    for s in range(sc):
        left = jnp.dot(hist[:, s * BINS:(s + 1) * BINS], upto, precision=lax.Precision.HIGHEST,
                       preferred_element_type=f32)
        left_grad, left_hess = left[:node_count], left[node_count:]
        total_grad, total_hess = left_grad[:, BINS - 1:], left_hess[:, BINS - 1:]
        gain = 0.5 * (left_grad * left_grad / (left_hess + l2_penalty)
                      + (total_grad - left_grad) ** 2 / (total_hess - left_hess + l2_penalty)
                      - total_grad * total_grad / (total_hess + l2_penalty))
        best.append(jnp.max(jnp.where(lane < BINS - 1, gain, low), axis=1, keepdims=True))
    half = sc // 2
    for s in range(half):
        best_out[:, s:s + 1] = jnp.where(core == 0, best[s], best[half + s])
    column = functools.reduce(jnp.maximum, best)
    diagonal = iota((node_count, LANES), 0) == iota((node_count, LANES), 1)
    top[...] = jnp.max(jnp.where(diagonal, column, low), axis=0, keepdims=True)

    copies = []
    for d in range(1, nz):
        copy = remote(top, top_z.at[d - 1], tz_send.at[d - 1], tz_recv.at[d - 1], at_z(d))
        copy.start()
        copies.append(copy)
    for copy in copies:
        copy.wait_recv()
    highest = top[...]
    for d in range(1, nz):
        highest = jnp.maximum(highest, top_z[d - 1])
    mid[...] = highest
    for i, (dx, dy) in enumerate(xy):
        copy = remote(mid, top_xy.at[i], txy_send.at[i], txy_recv.at[i], at_xy(dx, dy))
        copy.start()
        copies.append(copy)
    for copy in copies[nz - 1:]:
        copy.wait_recv()
    for i in range(len(xy)):
        highest = jnp.maximum(highest, top_xy[i])
    node_best_out[...] = highest[:, :node_count]

    for copy in copies + side_copies + [swap]:
        copy.wait_send()
    for d in range(1, nz):
        remote(outbox.at[0], zbox.at[d], z_send.at[d], z_recv.at[d], at_z(d)).wait_send()
    for d in range(nz):
        for copy in forwards(d):
            copy.wait_send()


def body(sizes, binned, gradients, hessians, parents, split_feature, split_bin, elected):
    ny, nz, nx = sizes
    rows_here, width = binned.shape
    node_count, slots_here = elected.shape
    chunks = rows_here // LANES
    sc = slots_here // (ny * nz)
    meta = jnp.stack([gradients.astype(f32), hessians.astype(f32), parents.astype(f32)]).reshape(3, chunks, LANES)
    vmem, smem = pl.BlockSpec(memory_space=pltpu.VMEM), pl.BlockSpec(memory_space=pltpu.SMEM)
    dma = pltpu.SemaphoreType.DMA
    nodes, best, node_best = pl.pallas_call(
        functools.partial(kernel, ny, nz, nx, sc),
        out_shape=(
            jax.ShapeDtypeStruct((chunks, LANES), i32),
            jax.ShapeDtypeStruct((node_count, sc // 2), f32),
            jax.ShapeDtypeStruct((1, node_count), f32),
        ),
        in_specs=[smem, smem, vmem, vmem, pl.BlockSpec(memory_space=pl.ANY)],
        out_specs=(vmem, vmem, vmem),
        scratch_shapes=[
            pltpu.VMEM((rows_here, width), i32),
            pltpu.VMEM((chunks, LANES), f32),
            pltpu.VMEM((nx - 1, chunks, LANES), f32),
            pltpu.VMEM((nz, 3 + ny * sc, chunks, LANES), f32),
            pltpu.VMEM((nz, 3 + ny * sc, chunks, LANES), f32),
            pltpu.VMEM((ny - 1, nz, 3 + sc, chunks, LANES), f32),
            pltpu.VMEM((2 * node_count, sc * BINS), f32),
            pltpu.VMEM((2 * node_count, sc * BINS), f32),
            pltpu.VMEM((1, LANES), f32),
            pltpu.VMEM((nz - 1, 1, LANES), f32),
            pltpu.VMEM((1, LANES), f32),
            pltpu.VMEM((nx * ny - 1, 1, LANES), f32),
            dma,
            dma((nx - 1,)), dma((nx - 1,)),
            dma((nz,)), dma((nz,)),
            dma((nz, ny - 1, 2)), dma((nz, ny - 1)),
            dma, dma,
            dma((nz - 1,)), dma((nz - 1,)),
            dma((nx * ny - 1,)), dma((nx * ny - 1,)),
        ],
        compiler_params=pltpu.CompilerParams(collective_id=0, has_side_effects=True),
        name="level",
    )(split_feature, split_bin, meta, elected, binned)
    return nodes.reshape(rows_here), best[:, None, :], node_best.reshape(node_count)


def solution(mesh):
    ny, nz, nx = 4, 8, mesh.shape["rep"]
    finer = Mesh(mesh.devices.reshape(ny, nz, 2, nx), ("rows_0", "rows_1", "rows_2", "rep"))
    placed = (P(ROWS, "rep"), P(ROWS), P(ROWS), P(ROWS), P(), P(), P(None, "rep"))
    return jax.shard_map(
        functools.partial(body, (ny, nz, nx)),
        mesh=finer,
        in_specs=placed,
        out_specs=(P(ROWS), P(None, "rep", ROWS), P()),
        check_vma=False,
    )
```

```python
import functools

import jax
import jax.numpy as jnp
from jax import lax
from jax.experimental import pallas as pl
from jax.experimental.pallas import tpu as pltpu
from jax.sharding import Mesh
from jax.sharding import PartitionSpec as P

BINS = 128
LANES = 128
ROWS = ("rows_0", "rows_1", "rows_2")
MESH_IDS = pl.DeviceIdType.MESH
f32, bf16, i32 = jnp.float32, jnp.bfloat16, jnp.int32

l2_penalty = 1.0


def iota(shape, dim, dtype=i32):
    out = lax.broadcasted_iota(i32, shape, dim)
    if dtype == bf16:
        return out.astype(f32).astype(bf16)
    return out.astype(dtype)


def remote(src, dst, send, recv, where):
    return pltpu.make_async_remote_copy(
        src_ref=src, dst_ref=dst, send_sem=send, recv_sem=recv, device_id=where, device_id_type=MESH_IDS
    )


def kernel(ny, nz, nx, sc, split_feature, split_bin, meta, elected, binned_hbm,
           nodes_out, best_out, node_best_out,
           binned, side, side_in, outbox, zbox, node_box, stats_box, weights, acc, acc_y, mine, acc_in,
           top, top_z, mid, top_xy,
           load_sem, side_send, side_recv, z_send, z_recv, node_send, node_recv, stats_send, stats_recv,
           y_send, y_recv, core_send, core_recv, tz_send, tz_recv, txy_send, txy_recv):
    y, z = lax.axis_index("rows_0"), lax.axis_index("rows_1")
    core, x = lax.axis_index("rows_2"), lax.axis_index("rep")
    parent_count = split_feature.shape[0]
    node_count = elected.shape[0]
    width = binned.shape[1]
    chunks = meta.shape[1]

    load = pltpu.make_async_copy(binned_hbm, binned, load_sem)
    load.start()

    def at_x(d):
        return {"rep": lax.rem(x + d, nx)}

    def at_y(d):
        return {"rows_0": lax.rem(y + d, ny)}

    def at_z(d):
        return {"rows_1": lax.rem(z + d, nz)}

    def at_xy(dx, dy):
        return {"rep": lax.rem(x + dx, nx), "rows_0": lax.rem(y + dy, ny)}

    def order(i):
        half, odd = (i + 1) // 2, i % 2
        return (odd * half + (1 - odd) * (nz - half)) % nz

    xy = [(dx, dy) for dx in range(nx) for dy in range(ny) if (dx, dy) != (0, 0)]
    peers = [at_z(d) for d in range(1, nz)] + [at_xy(*d) for d in xy] + [{"rows_2": 1 - core}]
    barrier = pltpu.get_barrier_semaphore()
    for peer in peers:
        pl.semaphore_signal(barrier, inc=1, device_id=peer, device_id_type=MESH_IDS)

    load.wait()
    parent_rows = iota((parent_count, LANES), 0)
    want = jnp.zeros((parent_count, width), i32)
    bound = jnp.zeros((parent_count, LANES), i32)
    for p in range(parent_count):
        want = jnp.where(iota((parent_count, width), 0) == p, split_feature[p] - x * width, want)
        bound = jnp.where(parent_rows == p, split_bin[p], bound)
    pick = jnp.where(iota((parent_count, width), 1) == want, jnp.ones((), f32), jnp.zeros((), f32)).astype(bf16)
    owned = (want[:, :LANES] >= 0) & (want[:, :LANES] < width)
    values = lax.dot_general(pick, binned[...].astype(f32).astype(bf16), (((1,), (1,)), ((), ())),
                             preferred_element_type=f32)
    bound = bound.astype(f32)
    for c in range(chunks):
        parent = meta[2, c:c + 1, :]
        hit = (parent_rows.astype(f32) == parent) & owned & (values[:, c * LANES:(c + 1) * LANES] > bound)
        side[c:c + 1, :] = jnp.max(jnp.where(hit, 1.0, 0.0), axis=0, keepdims=True)

    pl.semaphore_wait(barrier, len(peers))
    side_copies = []
    for d in range(1, nx):
        copy = remote(side, side_in.at[d - 1], side_send.at[d - 1], side_recv.at[d - 1], at_x(d))
        copy.start()
        side_copies.append(copy)
    stats = meta.at[0:2]
    for i in range(1, nz):
        d = order(i)
        remote(stats, stats_box.at[d], stats_send.at[d], stats_recv.at[d], at_z(d)).start()
    for copy in side_copies:
        copy.wait_recv()
    went = side[...]
    for d in range(1, nx):
        went = went + side_in[d - 1]
    node = 2.0 * meta[2] + went
    nodes_out[...] = node.astype(i32)

    chosen = elected[...].astype(f32).astype(bf16)
    node_rows = iota((node_count, LANES), 0).astype(f32)
    node_box[0] = node
    for c in range(chunks):
        hot = jnp.where(node_rows == node[c:c + 1, :], 1.0, 0.0).astype(bf16)
        index = lax.dot_general(hot, chosen, (((0,), (0,)), ((), ())), preferred_element_type=f32).astype(i32)
        inner = index & (LANES - 1)
        picked = None
        for b in range(width // LANES):
            part = jnp.take_along_axis(binned[c * LANES:(c + 1) * LANES, b * LANES:(b + 1) * LANES], inner, axis=1)
            picked = part if b == 0 else jnp.where(index >= b * LANES, part, picked)
        turned = picked.astype(f32).T
        for yy in range(ny):
            for zz in range(nz):
                first = (yy * nz + zz) * sc
                outbox[zz, yy, :, c, :] = turned[first:first + sc]
        if c == 1:
            for i in range(1, nz):
                d = order(i)
                remote(node_box.at[0], node_box.at[d], node_send.at[d], node_recv.at[d], at_z(d)).start()

    def bins_to(j, d):
        there = lax.rem(y + 1 + j, ny)
        return remote(outbox.at[lax.rem(z + d, nz), there], zbox.at[j, d], z_send.at[j, d], z_recv.at[j, d], at_z(d))

    for j in range(ny):
        for i in range(1, nz):
            bins_to(j, order(i)).start()

    def weigh(d):
        node_of = iota((node_count, LANES), 0, bf16)
        zero = jnp.zeros((), bf16)
        for c in range(chunks):
            here = node_of == node_box[d, c:c + 1, :].astype(bf16)
            at = slice(c * LANES, (c + 1) * LANES)
            weights[d, :node_count, at] = jnp.where(here, stats_box[d, 0, c:c + 1, :].astype(bf16), zero)
            weights[d, node_count:, at] = jnp.where(here, stats_box[d, 1, c:c + 1, :].astype(bf16), zero)

    def counted(box, d):
        bin_rows = iota((BINS, LANES), 0, bf16)
        one, zero = jnp.ones((), bf16), jnp.zeros((), bf16)
        hots = []
        for s in range(sc):
            row = [box[s, c:c + 1, :].astype(bf16) for c in range(chunks)]
            hots.append(jnp.concatenate([jnp.where(bin_rows == r, one, zero) for r in row], axis=1))
        return lax.dot_general(weights[d], jnp.concatenate(hots, axis=0), (((1,), (1,)), ((), ())),
                               preferred_element_type=f32)

    def wait_for(ref, sem):
        pltpu.make_async_copy(ref, ref, sem).wait()

    stats_box[0] = meta[0:2]
    weigh(0)

    def own(j, carry):
        acc[j] = counted(outbox.at[z, lax.rem(y + 1 + j, ny)], 0)
        return carry

    lax.fori_loop(0, ny, own, 0)

    def weigh_next(i, carry):
        d = order(i)
        wait_for(stats_box.at[d], stats_recv.at[d])
        wait_for(node_box.at[d], node_recv.at[d])
        weigh(d)
        return carry

    lax.fori_loop(1, nz, weigh_next, 0)

    def to_owner(j):
        return remote(acc.at[j], acc_y.at[j], y_send.at[j], y_recv.at[j], at_y(1 + j))

    def add_group(j, group):
        for d in group:
            wait_for(zbox.at[j, d], z_recv.at[j, d])
        acc[j] += functools.reduce(jnp.add, [counted(zbox.at[j, d], d) for d in group])

    groups = [[order(i) for i in range(1, nz)][k:k + 4] for k in range(0, nz - 1, 4)]

    def next_round(j, carry):
        add_group(j, groups[0])

        @pl.when(j > 0)
        def _():
            to_owner(j - 1).start()

        for group in groups[1:]:
            add_group(j, group)
        return carry

    lax.fori_loop(0, ny, next_round, 0)
    total = acc[ny - 1]
    for j in range(ny - 1):
        to_owner(j).wait_recv()
        total = total + acc_y[j]
    mine[...] = total

    swap = remote(mine, acc_in, core_send, core_recv, {"rows_2": 1 - core})
    swap.start()
    swap.wait_recv()
    hist = total + acc_in[...]
    upto = jnp.where(iota((BINS, BINS), 0) <= iota((BINS, BINS), 1), 1.0, 0.0)
    lane = iota((node_count, BINS), 1)
    low = jnp.full((), -3.0e38, f32)
    best = []
    for s in range(sc):
        left = jnp.dot(hist[:, s * BINS:(s + 1) * BINS], upto, precision=lax.Precision.HIGHEST,
                       preferred_element_type=f32)
        left_grad, left_hess = left[:node_count], left[node_count:]
        total_grad, total_hess = left_grad[:, BINS - 1:], left_hess[:, BINS - 1:]
        gain = 0.5 * (left_grad * left_grad / (left_hess + l2_penalty)
                      + (total_grad - left_grad) ** 2 / (total_hess - left_hess + l2_penalty)
                      - total_grad * total_grad / (total_hess + l2_penalty))
        best.append(jnp.max(jnp.where(lane < BINS - 1, gain, low), axis=1, keepdims=True))
    half = sc // 2
    for s in range(half):
        best_out[:, s:s + 1] = jnp.where(core == 0, best[s], best[half + s])
    column = functools.reduce(jnp.maximum, best)
    diagonal = iota((node_count, LANES), 0) == iota((node_count, LANES), 1)
    top[...] = jnp.max(jnp.where(diagonal, column, low), axis=0, keepdims=True)

    copies = []
    for d in range(1, nz):
        copy = remote(top, top_z.at[d - 1], tz_send.at[d - 1], tz_recv.at[d - 1], at_z(d))
        copy.start()
        copies.append(copy)
    for copy in copies:
        copy.wait_recv()
    highest = top[...]
    for d in range(1, nz):
        highest = jnp.maximum(highest, top_z[d - 1])
    mid[...] = highest
    for i, (dx, dy) in enumerate(xy):
        copy = remote(mid, top_xy.at[i], txy_send.at[i], txy_recv.at[i], at_xy(dx, dy))
        copy.start()
        copies.append(copy)
    for copy in copies[nz - 1:]:
        copy.wait_recv()
    for i in range(len(xy)):
        highest = jnp.maximum(highest, top_xy[i])
    node_best_out[...] = highest[:, :node_count]

    for copy in copies + side_copies + [swap]:
        copy.wait_send()
    for d in range(1, nz):
        remote(stats, stats_box.at[d], stats_send.at[d], stats_recv.at[d], at_z(d)).wait_send()
        remote(node_box.at[0], node_box.at[d], node_send.at[d], node_recv.at[d], at_z(d)).wait_send()
        for j in range(ny):
            bins_to(j, d).wait_send()
    for j in range(ny - 1):
        to_owner(j).wait_send()


def body(sizes, binned, gradients, hessians, parents, split_feature, split_bin, elected):
    ny, nz, nx = sizes
    rows_here, width = binned.shape
    node_count, slots_here = elected.shape
    chunks = rows_here // LANES
    sc = slots_here // (ny * nz)
    meta = jnp.stack([gradients.astype(f32), hessians.astype(f32), parents.astype(f32)]).reshape(3, chunks, LANES)
    vmem, smem = pl.BlockSpec(memory_space=pltpu.VMEM), pl.BlockSpec(memory_space=pltpu.SMEM)
    dma = pltpu.SemaphoreType.DMA
    nodes, best, node_best = pl.pallas_call(
        functools.partial(kernel, ny, nz, nx, sc),
        out_shape=(
            jax.ShapeDtypeStruct((chunks, LANES), i32),
            jax.ShapeDtypeStruct((node_count, sc // 2), f32),
            jax.ShapeDtypeStruct((1, node_count), f32),
        ),
        in_specs=[smem, smem, vmem, vmem, pl.BlockSpec(memory_space=pl.ANY)],
        out_specs=(vmem, vmem, vmem),
        scratch_shapes=[
            pltpu.VMEM((rows_here, width), i32),
            pltpu.VMEM((chunks, LANES), f32),
            pltpu.VMEM((nx - 1, chunks, LANES), f32),
            pltpu.VMEM((nz, ny, sc, chunks, LANES), f32),
            pltpu.VMEM((ny, nz, sc, chunks, LANES), f32),
            pltpu.VMEM((nz, chunks, LANES), f32),
            pltpu.VMEM((nz, 2, chunks, LANES), f32),
            pltpu.VMEM((nz, 2 * node_count, rows_here), bf16),
            pltpu.VMEM((ny, 2 * node_count, sc * BINS), f32),
            pltpu.VMEM((ny - 1, 2 * node_count, sc * BINS), f32),
            pltpu.VMEM((2 * node_count, sc * BINS), f32),
            pltpu.VMEM((2 * node_count, sc * BINS), f32),
            pltpu.VMEM((1, LANES), f32),
            pltpu.VMEM((nz - 1, 1, LANES), f32),
            pltpu.VMEM((1, LANES), f32),
            pltpu.VMEM((nx * ny - 1, 1, LANES), f32),
            dma,
            dma((nx - 1,)), dma((nx - 1,)),
            dma((ny, nz)), dma((ny, nz)),
            dma((nz,)), dma((nz,)),
            dma((nz,)), dma((nz,)),
            dma((ny - 1,)), dma((ny - 1,)),
            dma, dma,
            dma((nz - 1,)), dma((nz - 1,)),
            dma((nx * ny - 1,)), dma((nx * ny - 1,)),
        ],
        compiler_params=pltpu.CompilerParams(collective_id=0, has_side_effects=True),
        name="level",
    )(split_feature, split_bin, meta, elected, binned)
    return nodes.reshape(rows_here), best[:, None, :], node_best.reshape(node_count)


def solution(mesh):
    ny, nz, nx = 4, 8, mesh.shape["rep"]
    finer = Mesh(mesh.devices.reshape(ny, nz, 2, nx), ("rows_0", "rows_1", "rows_2", "rep"))
    placed = (P(ROWS, "rep"), P(ROWS), P(ROWS), P(ROWS), P(), P(), P(None, "rep"))
    return jax.shard_map(
        functools.partial(body, (ny, nz, nx)),
        mesh=finer,
        in_specs=placed,
        out_specs=(P(ROWS), P(None, "rep", ROWS), P()),
        check_vma=False,
    )
```

```python
import functools

import jax
import jax.numpy as jnp
from jax import lax
from jax.experimental import pallas as pl
from jax.experimental.pallas import tpu as pltpu
from jax.sharding import Mesh
from jax.sharding import PartitionSpec as P

BINS = 128
LANES = 128
ROWS = ("rows_0", "rows_1", "rows_2")
MESH_IDS = pl.DeviceIdType.MESH
f32, bf16, i32, f8 = jnp.float32, jnp.bfloat16, jnp.int32, jnp.float8_e4m3fn

l2_penalty = 1.0


def iota(shape, dim, dtype=i32):
    out = lax.broadcasted_iota(i32, shape, dim)
    if dtype == bf16:
        return out.astype(f32).astype(bf16)
    return out.astype(dtype)


def remote(src, dst, send, recv, where):
    return pltpu.make_async_remote_copy(
        src_ref=src, dst_ref=dst, send_sem=send, recv_sem=recv, device_id=where, device_id_type=MESH_IDS
    )


def kernel(ny, nz, nx, sc, split_feature, split_bin, gradients, hessians, parents, elected, binned_hbm,
           nodes_out, best_out, node_best_out,
           binned, side, side_in, left_box, outbox, zbox, node_box, stats_box, weights, acc, acc_y, mine, acc_in,
           top, tops,
           load_sem, side_send, side_recv, z_send, z_recv, node_send, node_recv, stats_send, stats_recv,
           y_send, y_recv, core_send, core_recv, top_send, top_recv):
    y, z = lax.axis_index("rows_0"), lax.axis_index("rows_1")
    core, x = lax.axis_index("rows_2"), lax.axis_index("rep")
    parent_count = split_feature.shape[0]
    node_count = elected.shape[0]
    width = binned.shape[1]
    chunks = parents.shape[0]

    load = pltpu.make_async_copy(binned_hbm, binned, load_sem)
    load.start()

    def at_x(d):
        return {"rep": lax.rem(x + d, nx)}

    def at_y(d):
        return {"rows_0": lax.rem(y + d, ny)}

    def at_z(d):
        return {"rows_1": lax.rem(z + d, nz)}

    def at_xy(dx, dy):
        return {"rep": lax.rem(x + dx, nx), "rows_0": lax.rem(y + dy, ny)}

    def order(i):
        half, odd = (i + 1) // 2, i % 2
        return (odd * half + (1 - odd) * (nz - half)) % nz

    xy = [(dx, dy) for dx in range(nx) for dy in range(ny) if (dx, dy) != (0, 0)]
    peers = [at_z(d) for d in range(1, nz)] + [at_xy(*d) for d in xy] + [{"rows_2": 1 - core}]
    barrier = pltpu.get_barrier_semaphore()
    for peer in peers:
        pl.semaphore_signal(barrier, inc=1, device_id=peer, device_id_type=MESH_IDS)

    stats_box[0, 0] = gradients[...].astype(f32)
    stats_box[0, 1] = hessians[...].astype(f32)
    parent = parents[...].astype(f32)

    load.wait()
    parent_rows = iota((parent_count, LANES), 0)
    want = jnp.zeros((parent_count, width), i32)
    bound = jnp.zeros((parent_count, LANES), i32)
    for p in range(parent_count):
        want = jnp.where(iota((parent_count, width), 0) == p, split_feature[p] - x * width, want)
        bound = jnp.where(parent_rows == p, split_bin[p], bound)
    pick = jnp.where(iota((parent_count, width), 1) == want, jnp.ones((), f32), jnp.zeros((), f32)).astype(bf16)
    owned = (want[:, :LANES] >= 0) & (want[:, :LANES] < width)
    values = lax.dot_general(pick, binned[...].astype(f32).astype(bf16), (((1,), (1,)), ((), ())),
                             preferred_element_type=f32)
    bound = bound.astype(f32)
    for c in range(chunks):
        hit = (parent_rows.astype(f32) == parent[c:c + 1]) & owned & (values[:, c * LANES:(c + 1) * LANES] > bound)
        side[c:c + 1, :] = jnp.max(jnp.where(hit, 1.0, 0.0), axis=0, keepdims=True)

    pl.semaphore_wait(barrier, len(peers))
    side_copies = []
    for d in range(1, nx):
        copy = remote(side, side_in.at[d - 1], side_send.at[d - 1], side_recv.at[d - 1], at_x(d))
        copy.start()
        side_copies.append(copy)
    stats = stats_box.at[0]
    for i in range(1, nz):
        d = order(i)
        remote(stats, stats_box.at[d], stats_send.at[d], stats_recv.at[d], at_z(d)).start()
    chosen = elected[...].astype(f32).astype(bf16)
    node_rows = iota((node_count, LANES), 0).astype(f32)
    for c in range(chunks):
        rows = slice(c * LANES, (c + 1) * LANES)
        packed = binned[rows, :LANES]
        for b in range(1, width // LANES):
            packed = packed + (binned[rows, b * LANES:(b + 1) * LANES] << (8 * b))
        for way, box in ((0, left_box), (1, outbox)):
            hot = jnp.where(node_rows == 2.0 * parent[c:c + 1] + way, 1.0, 0.0).astype(bf16)
            index = lax.dot_general(hot, chosen, (((0,), (0,)), ((), ())), preferred_element_type=f32).astype(i32)
            found = jnp.take_along_axis(packed, index & (LANES - 1), axis=1, mode="promise_in_bounds")
            found = (found >> ((index >> 7) << 3)) & (BINS - 1)
            turned = found.astype(f32).T
            for yy in range(ny):
                for zz in range(nz):
                    first = (yy * nz + zz) * sc
                    box[zz, yy, :, c, :] = turned[first:first + sc]

    for copy in side_copies:
        copy.wait_recv()
    went = side[...]
    for d in range(1, nx):
        went = went + side_in[d - 1]
    node = 2.0 * parent + went
    nodes_out[...] = node.astype(i32)
    node_box[0] = node
    right = (went > 0.0)[None]
    for yy in range(ny):
        for zz in range(nz):
            outbox[zz, yy] = jnp.where(right, outbox[zz, yy], left_box[zz, yy])
    for i in range(1, nz):
        d = order(i)
        remote(node_box.at[0], node_box.at[d], node_send.at[d], node_recv.at[d], at_z(d)).start()

    def bins_to(j, d):
        there = lax.rem(y + 1 + j, ny)
        return remote(outbox.at[lax.rem(z + d, nz), there], zbox.at[j, d], z_send.at[j, d], z_recv.at[j, d], at_z(d))

    for j in range(ny):
        for i in range(1, nz):
            bins_to(j, order(i)).start()

    def weigh(d):
        node_of = iota((node_count, LANES), 0, bf16)
        zero = jnp.zeros((), bf16)
        for c in range(chunks):
            here = node_of == node_box[d, c:c + 1, :].astype(bf16)
            at = slice(c * LANES, (c + 1) * LANES)
            weights[d, :node_count, at] = jnp.where(here, stats_box[d, 0, c:c + 1, :].astype(bf16), zero)
            weights[d, node_count:, at] = jnp.where(here, stats_box[d, 1, c:c + 1, :].astype(bf16), zero)

    def counted(box, d):
        bin_rows = iota((BINS, LANES), 0, bf16)
        one, zero = jnp.ones((), bf16), jnp.zeros((), bf16)
        hots = []
        for s in range(sc):
            row = [box[s, c:c + 1, :].astype(bf16) for c in range(chunks)]
            hots.append(jnp.concatenate([jnp.where(bin_rows == r, one, zero) for r in row], axis=1))
        return lax.dot_general(weights[d], jnp.concatenate(hots, axis=0).astype(f8), (((1,), (1,)), ((), ())),
                               preferred_element_type=f32)

    def wait_for(ref, sem):
        pltpu.make_async_copy(ref, ref, sem).wait()

    weigh(0)

    def own(j, carry):
        acc[j] = counted(outbox.at[z, lax.rem(y + 1 + j, ny)], 0)
        return carry

    lax.fori_loop(0, ny, own, 0)

    def weigh_next(i, carry):
        d = order(i)
        wait_for(stats_box.at[d], stats_recv.at[d])
        wait_for(node_box.at[d], node_recv.at[d])
        weigh(d)
        return carry

    lax.fori_loop(1, nz, weigh_next, 0)

    def to_owner(j):
        return remote(acc.at[j], acc_y.at[j], y_send.at[j], y_recv.at[j], at_y(1 + j))

    def add_group(j, group):
        for d in group:
            wait_for(zbox.at[j, d], z_recv.at[j, d])
        acc[j] += functools.reduce(jnp.add, [counted(zbox.at[j, d], d) for d in group])

    groups = [[order(i) for i in range(1, nz)][k:k + 4] for k in range(0, nz - 1, 4)]

    def next_round(j, carry):
        for group in groups:
            add_group(j, group)

        @pl.when(j < ny - 1)
        def _():
            to_owner(j).start()

        return carry

    lax.fori_loop(0, ny, next_round, 0)
    total = acc[ny - 1]
    for j in range(ny - 1):
        to_owner(j).wait_recv()
        total = total + acc_y[j]
    mine[...] = total

    swap = remote(mine, acc_in, core_send, core_recv, {"rows_2": 1 - core})
    swap.start()
    swap.wait_recv()
    hist = total + acc_in[...]
    upto = jnp.where(iota((BINS, BINS), 0) <= iota((BINS, BINS), 1), 1.0, 0.0)
    lane = iota((node_count, BINS), 1)
    low = jnp.full((), -3.0e38, f32)
    best = []
    for s in range(sc):
        left = jnp.dot(hist[:, s * BINS:(s + 1) * BINS], upto, precision=lax.Precision.HIGHEST,
                       preferred_element_type=f32)
        left_grad, left_hess = left[:node_count], left[node_count:]
        total_grad, total_hess = left_grad[:, BINS - 1:], left_hess[:, BINS - 1:]
        gain = 0.5 * (left_grad * left_grad / (left_hess + l2_penalty)
                      + (total_grad - left_grad) ** 2 / (total_hess - left_hess + l2_penalty)
                      - total_grad * total_grad / (total_hess + l2_penalty))
        best.append(jnp.max(jnp.where(lane < BINS - 1, gain, low), axis=1, keepdims=True))
    half = sc // 2
    diagonal = iota((node_count, LANES), 0) == iota((node_count, LANES), 1)

    def across(column):
        return jnp.max(jnp.where(diagonal, column, low), axis=0, keepdims=True)

    top[...] = across(functools.reduce(jnp.maximum, best))
    for s in range(half):
        best_out[s:s + 1] = across(jnp.where(core == 0, best[s], best[half + s]))[:, :node_count]

    others = [(dx, dy, dz) for dx in range(nx) for dy in range(ny) for dz in range(nz)][1:]
    far = {n: [min(k, n - k) for k in range(n)] for n in (nx, ny, nz)}
    others.sort(key=lambda d: -(far[nx][d[0]] + far[ny][d[1]] + far[nz][d[2]]))
    for i, (dx, dy, dz) in enumerate(others):
        remote(top, tops.at[i], top_send, top_recv,
               {"rep": lax.rem(x + dx, nx), "rows_0": lax.rem(y + dy, ny), "rows_1": lax.rem(z + dz, nz)}).start()
    wait_for(tops, top_recv)
    node_best_out[...] = jnp.maximum(top[...], jnp.max(tops[...], axis=0))[:, :node_count]

    for copy in side_copies + [swap]:
        copy.wait_send()
    wait_for(tops, top_send)
    for d in range(1, nz):
        remote(stats, stats_box.at[d], stats_send.at[d], stats_recv.at[d], at_z(d)).wait_send()
        remote(node_box.at[0], node_box.at[d], node_send.at[d], node_recv.at[d], at_z(d)).wait_send()
        for j in range(ny):
            bins_to(j, d).wait_send()
    for j in range(ny - 1):
        to_owner(j).wait_send()


def body(sizes, binned, gradients, hessians, parents, split_feature, split_bin, elected):
    ny, nz, nx = sizes
    rows_here, width = binned.shape
    node_count, slots_here = elected.shape
    chunks = rows_here // LANES
    sc = slots_here // (ny * nz)
    shape = (chunks, LANES)
    vmem, smem = pl.BlockSpec(memory_space=pltpu.VMEM), pl.BlockSpec(memory_space=pltpu.SMEM)
    dma = pltpu.SemaphoreType.DMA
    nodes, best, node_best = pl.pallas_call(
        functools.partial(kernel, ny, nz, nx, sc),
        out_shape=(
            jax.ShapeDtypeStruct((chunks, LANES), i32),
            jax.ShapeDtypeStruct((sc // 2, node_count), f32),
            jax.ShapeDtypeStruct((1, node_count), f32),
        ),
        in_specs=[smem, smem, vmem, vmem, vmem, vmem, pl.BlockSpec(memory_space=pl.ANY)],
        out_specs=(vmem, vmem, vmem),
        scratch_shapes=[
            pltpu.VMEM((rows_here, width), i32),
            pltpu.VMEM((chunks, LANES), f32),
            pltpu.VMEM((nx - 1, chunks, LANES), f32),
            pltpu.VMEM((nz, ny, sc, chunks, LANES), f32),
            pltpu.VMEM((nz, ny, sc, chunks, LANES), f32),
            pltpu.VMEM((ny, nz, sc, chunks, LANES), f32),
            pltpu.VMEM((nz, chunks, LANES), f32),
            pltpu.VMEM((nz, 2, chunks, LANES), f32),
            pltpu.VMEM((nz, 2 * node_count, rows_here), bf16),
            pltpu.VMEM((ny, 2 * node_count, sc * BINS), f32),
            pltpu.VMEM((ny - 1, 2 * node_count, sc * BINS), f32),
            pltpu.VMEM((2 * node_count, sc * BINS), f32),
            pltpu.VMEM((2 * node_count, sc * BINS), f32),
            pltpu.VMEM((1, LANES), f32),
            pltpu.VMEM((nx * ny * nz - 1, 1, LANES), f32),
            dma,
            dma((nx - 1,)), dma((nx - 1,)),
            dma((ny, nz)), dma((ny, nz)),
            dma((nz,)), dma((nz,)),
            dma((nz,)), dma((nz,)),
            dma((ny - 1,)), dma((ny - 1,)),
            dma, dma,
            dma, dma,
        ],
        compiler_params=pltpu.CompilerParams(collective_id=0, has_side_effects=True),
        name="level",
    )(split_feature, split_bin, gradients.reshape(shape), hessians.reshape(shape), parents.reshape(shape), elected, binned)
    return nodes.reshape(rows_here), best.T[:, None, :], node_best.reshape(node_count)


def solution(mesh):
    ny, nz, nx = 4, 8, mesh.shape["rep"]
    finer = Mesh(mesh.devices.reshape(ny, nz, 2, nx), ("rows_0", "rows_1", "rows_2", "rep"))
    placed = (P(ROWS, "rep"), P(ROWS), P(ROWS), P(ROWS), P(), P(), P(None, "rep"))
    return jax.shard_map(
        functools.partial(body, (ny, nz, nx)),
        mesh=finer,
        in_specs=placed,
        out_specs=(P(ROWS), P(None, "rep", ROWS), P()),
        check_vma=False,
    )
```

```python
import functools

import jax
import jax.numpy as jnp
from jax import lax
from jax.experimental import pallas as pl
from jax.experimental.pallas import tpu as pltpu
from jax.sharding import Mesh
from jax.sharding import PartitionSpec as P

BINS = 128
LANES = 128
ROWS = ("rows_0", "rows_1", "rows_2")
MESH_IDS = pl.DeviceIdType.MESH
f32, bf16, i32, f8 = jnp.float32, jnp.bfloat16, jnp.int32, jnp.float8_e4m3fn

l2_penalty = 1.0


def iota(shape, dim, dtype=i32):
    out = lax.broadcasted_iota(i32, shape, dim)
    if dtype == bf16:
        return out.astype(f32).astype(bf16)
    return out.astype(dtype)


def remote(src, dst, send, recv, where):
    return pltpu.make_async_remote_copy(
        src_ref=src, dst_ref=dst, send_sem=send, recv_sem=recv, device_id=where, device_id_type=MESH_IDS
    )


def kernel(ny, nz, nx, sc, split_feature_hbm, split_bin_hbm, gradients_hbm, hessians_hbm, parents_hbm, elected_hbm, binned_hbm,
           nodes_out, best_out, node_best_out,
           split_feature, split_bin, gradients, hessians, parents, elected, binned, side, side_in, left_box, outbox, zbox, node_box, stats_box, weights, acc, acc_y, mine, acc_in,
           top, tops,
           load_sems, side_send, side_recv, z_send, z_recv, node_send, node_recv, stats_send, stats_recv,
           y_send, y_recv, core_send, core_recv, top_send, top_recv):
    y, z = lax.axis_index("rows_0"), lax.axis_index("rows_1")
    core, x = lax.axis_index("rows_2"), lax.axis_index("rep")
    parent_count = split_feature.shape[0]
    node_count = elected.shape[0]
    width = binned.shape[1]
    chunks = parents.shape[0]

    pairs = ((binned_hbm, binned), (parents_hbm, parents), (split_feature_hbm, split_feature), (split_bin_hbm, split_bin),
             (gradients_hbm, gradients), (hessians_hbm, hessians), (elected_hbm, elected))
    loads = [pltpu.make_async_copy(src, dst, load_sems.at[i]) for i, (src, dst) in enumerate(pairs)]
    for load in loads:
        load.start()

    def at_x(d):
        return {"rep": lax.rem(x + d, nx)}

    def at_y(d):
        return {"rows_0": lax.rem(y + d, ny)}

    def at_z(d):
        return {"rows_1": lax.rem(z + d, nz), "rows_2": 1 - core}

    def at_xy(dx, dy):
        return {"rep": lax.rem(x + dx, nx), "rows_0": lax.rem(y + dy, ny)}

    def order(i):
        half, odd = (i + 1) // 2, i % 2
        return (odd * half + (1 - odd) * (nz - half)) % nz

    xy = [(dx, dy) for dx in range(nx) for dy in range(ny) if (dx, dy) != (0, 0)]
    peers = [at_z(d) for d in range(1, nz)] + [at_xy(*d) for d in xy] + [{"rows_2": 1 - core}]
    barrier = pltpu.get_barrier_semaphore()
    for peer in peers:
        pl.semaphore_signal(barrier, inc=1, device_id=peer, device_id_type=MESH_IDS)

    for load in loads[1:]:
        load.wait()
    stats_box[0, 0] = gradients[...].astype(f32)
    stats_box[0, 1] = hessians[...].astype(f32)
    parent = parents[...].astype(f32)
    parent_rows = iota((parent_count, LANES), 0)
    want = jnp.zeros((parent_count, width), i32)
    bound = jnp.zeros((parent_count, LANES), i32)
    for p in range(parent_count):
        want = jnp.where(iota((parent_count, width), 0) == p, split_feature[p] - x * width, want)
        bound = jnp.where(parent_rows == p, split_bin[p], bound)
    pick = jnp.where(iota((parent_count, width), 1) == want, jnp.ones((), f32), jnp.zeros((), f32)).astype(bf16)
    owned = (want[:, :LANES] >= 0) & (want[:, :LANES] < width)
    loads[0].wait()
    values = lax.dot_general(pick, binned[...].astype(f32).astype(bf16), (((1,), (1,)), ((), ())),
                             preferred_element_type=f32)
    bound = bound.astype(f32)
    for c in range(chunks):
        hit = (parent_rows.astype(f32) == parent[c:c + 1]) & owned & (values[:, c * LANES:(c + 1) * LANES] > bound)
        side[c:c + 1, :] = jnp.max(jnp.where(hit, 1.0, 0.0), axis=0, keepdims=True)

    pl.semaphore_wait(barrier, len(peers))
    side_copies = []
    for d in range(1, nx):
        copy = remote(side, side_in.at[d - 1], side_send.at[d - 1], side_recv.at[d - 1], at_x(d))
        copy.start()
        side_copies.append(copy)
    stats = stats_box.at[0]
    for i in range(1, nz):
        d = order(i)
        remote(stats, stats_box.at[d], stats_send.at[d], stats_recv.at[d], at_z(d)).start()
    chosen = elected[...].astype(f32).astype(bf16)
    node_rows = iota((node_count, LANES), 0).astype(f32)
    for c in range(chunks):
        rows = slice(c * LANES, (c + 1) * LANES)
        packed = binned[rows, :LANES]
        for b in range(1, width // LANES):
            packed = packed + (binned[rows, b * LANES:(b + 1) * LANES] << (8 * b))
        for way, box in ((0, left_box), (1, outbox)):
            hot = jnp.where(node_rows == 2.0 * parent[c:c + 1] + way, 1.0, 0.0).astype(bf16)
            index = lax.dot_general(hot, chosen, (((0,), (0,)), ((), ())), preferred_element_type=f32).astype(i32)
            found = jnp.take_along_axis(packed, index & (LANES - 1), axis=1, mode="promise_in_bounds")
            found = (found >> ((index >> 7) << 3)) & (BINS - 1)
            turned = found.astype(f32).T
            for yy in range(ny):
                for zz in range(nz):
                    first = (yy * nz + zz) * sc
                    box[zz, yy, :, c, :] = turned[first:first + sc]

    for copy in side_copies:
        copy.wait_recv()
    went = side[...]
    for d in range(1, nx):
        went = went + side_in[d - 1]
    node = 2.0 * parent + went
    nodes_out[...] = node.astype(i32)
    node_box[0] = node
    right = (went > 0.0)[None]
    for yy in range(ny):
        for zz in range(nz):
            outbox[zz, yy] = jnp.where(right, outbox[zz, yy], left_box[zz, yy])
    for i in range(1, nz):
        d = order(i)
        remote(node_box.at[0], node_box.at[d], node_send.at[d], node_recv.at[d], at_z(d)).start()

    def bins_to(j, d):
        there = lax.rem(y + 1 + j, ny)
        return remote(outbox.at[lax.rem(z + d, nz), there], zbox.at[j, d], z_send.at[j, d], z_recv.at[j, d], at_z(d))

    for j in range(ny):
        for i in range(1, nz):
            bins_to(j, order(i)).start()

    def weigh(d):
        node_of = iota((node_count, LANES), 0, bf16)
        zero = jnp.zeros((), bf16)
        for c in range(chunks):
            here = node_of == node_box[d, c:c + 1, :].astype(bf16)
            at = slice(c * LANES, (c + 1) * LANES)
            weights[d, :node_count, at] = jnp.where(here, stats_box[d, 0, c:c + 1, :].astype(bf16), zero)
            weights[d, node_count:, at] = jnp.where(here, stats_box[d, 1, c:c + 1, :].astype(bf16), zero)

    def counted(box, d):
        bin_rows = iota((BINS, LANES), 0, bf16)
        one, zero = jnp.ones((), bf16), jnp.zeros((), bf16)
        hots = []
        for s in range(sc):
            row = [box[s, c:c + 1, :].astype(bf16) for c in range(chunks)]
            hots.append(jnp.concatenate([jnp.where(bin_rows == r, one, zero) for r in row], axis=1))
        return lax.dot_general(weights[d], jnp.concatenate(hots, axis=0).astype(f8), (((1,), (1,)), ((), ())),
                               preferred_element_type=f32)

    def wait_for(ref, sem):
        pltpu.make_async_copy(ref, ref, sem).wait()

    weigh(0)

    def own(j, carry):
        acc[j] = counted(outbox.at[z, lax.rem(y + 1 + j, ny)], 0)
        return carry

    lax.fori_loop(0, ny, own, 0)

    def to_owner(j):
        return remote(acc.at[j], acc_y.at[j], y_send.at[j], y_recv.at[j], at_y(1 + j))

    def add_group(j, group):
        for d in group:
            wait_for(zbox.at[j, d], z_recv.at[j, d])
        acc[j] += functools.reduce(jnp.add, [counted(zbox.at[j, d], d) for d in group])

    ranked = [order(i) for i in range(1, nz)]
    for k in range(0, nz - 1, 2):
        for d in ranked[k:k + 2]:
            wait_for(stats_box.at[d], stats_recv.at[d])
            wait_for(node_box.at[d], node_recv.at[d])
            weigh(d)
        add_group(0, ranked[k:k + 2])
    to_owner(0).start()

    def next_round(j, carry):
        for k in range(0, nz - 1, 4):
            add_group(j, ranked[k:k + 4])

        @pl.when(j < ny - 1)
        def _():
            to_owner(j).start()

        return carry

    lax.fori_loop(1, ny, next_round, 0)
    total = acc[ny - 1]
    for j in range(ny - 1):
        to_owner(j).wait_recv()
        total = total + acc_y[j]
    mine[...] = total

    swap = remote(mine, acc_in, core_send, core_recv, {"rows_2": 1 - core})
    swap.start()
    swap.wait_recv()
    hist = total + acc_in[...]
    upto = jnp.where(iota((BINS, BINS), 0) <= iota((BINS, BINS), 1), 1.0, 0.0)
    lane = iota((node_count, BINS), 1)
    low = jnp.full((), -3.0e38, f32)
    best = []
    for s in range(sc):
        left = jnp.dot(hist[:, s * BINS:(s + 1) * BINS], upto, precision=lax.Precision.HIGHEST,
                       preferred_element_type=f32)
        left_grad, left_hess = left[:node_count], left[node_count:]
        total_grad, total_hess = left_grad[:, BINS - 1:], left_hess[:, BINS - 1:]
        gain = 0.5 * (left_grad * left_grad / (left_hess + l2_penalty)
                      + (total_grad - left_grad) ** 2 / (total_hess - left_hess + l2_penalty)
                      - total_grad * total_grad / (total_hess + l2_penalty))
        best.append(jnp.max(jnp.where(lane < BINS - 1, gain, low), axis=1, keepdims=True))
    half = sc // 2
    diagonal = iota((node_count, LANES), 0) == iota((node_count, LANES), 1)

    def across(column):
        return jnp.max(jnp.where(diagonal, column, low), axis=0, keepdims=True)

    top[...] = across(functools.reduce(jnp.maximum, best))
    for s in range(half):
        best_out[s:s + 1] = across(jnp.where(core == 0, best[s], best[half + s]))[:, :node_count]

    others = [(dx, dy, dz) for dx in range(nx) for dy in range(ny) for dz in range(nz)][1:]
    far = {n: [min(k, n - k) for k in range(n)] for n in (nx, ny, nz)}
    others.sort(key=lambda d: -(far[nx][d[0]] + far[ny][d[1]] + far[nz][d[2]]))
    for i, (dx, dy, dz) in enumerate(others):
        remote(top, tops.at[i], top_send, top_recv,
               {"rep": lax.rem(x + dx, nx), "rows_0": lax.rem(y + dy, ny), "rows_1": lax.rem(z + dz, nz),
                "rows_2": 1 - core}).start()
    wait_for(tops, top_recv)
    node_best_out[...] = jnp.maximum(top[...], jnp.max(tops[...], axis=0))[:, :node_count]

    for copy in side_copies + [swap]:
        copy.wait_send()
    wait_for(tops, top_send)
    for d in range(1, nz):
        remote(stats, stats_box.at[d], stats_send.at[d], stats_recv.at[d], at_z(d)).wait_send()
        remote(node_box.at[0], node_box.at[d], node_send.at[d], node_recv.at[d], at_z(d)).wait_send()
        for j in range(ny):
            bins_to(j, d).wait_send()
    for j in range(ny - 1):
        to_owner(j).wait_send()


def finish(nodes, best, node_best, nodes_out, best_out, node_best_out):
    nodes_out[...] = nodes[...]
    best_out[...] = best[...]
    node_best_out[...] = node_best[...]


def body(sizes, binned, gradients, hessians, parents, split_feature, split_bin, elected):
    ny, nz, nx = sizes
    rows_here, width = binned.shape
    node_count, slots_here = elected.shape
    chunks = rows_here // LANES
    sc = slots_here // (ny * nz)
    shape = (chunks, LANES)
    vmem = pl.BlockSpec(memory_space=pltpu.VMEM)
    dma = pltpu.SemaphoreType.DMA
    results = (
        jax.ShapeDtypeStruct((chunks, LANES), i32),
        jax.ShapeDtypeStruct((sc // 2, node_count), f32),
        jax.ShapeDtypeStruct((1, node_count), f32),
    )
    outs = pl.pallas_call(
        functools.partial(kernel, ny, nz, nx, sc),
        out_shape=results,
        in_specs=[pl.BlockSpec(memory_space=pl.ANY)] * 7,
        out_specs=(vmem, vmem, vmem),
        scratch_shapes=[
            pltpu.SMEM(split_feature.shape, i32),
            pltpu.SMEM(split_bin.shape, i32),
            pltpu.VMEM(shape, bf16),
            pltpu.VMEM(shape, bf16),
            pltpu.VMEM(shape, i32),
            pltpu.VMEM(elected.shape, i32),
            pltpu.VMEM((rows_here, width), i32),
            pltpu.VMEM((chunks, LANES), f32),
            pltpu.VMEM((nx - 1, chunks, LANES), f32),
            pltpu.VMEM((nz, ny, sc, chunks, LANES), f32),
            pltpu.VMEM((nz, ny, sc, chunks, LANES), f32),
            pltpu.VMEM((ny, nz, sc, chunks, LANES), f32),
            pltpu.VMEM((nz, chunks, LANES), f32),
            pltpu.VMEM((nz, 2, chunks, LANES), f32),
            pltpu.VMEM((nz, 2 * node_count, rows_here), bf16),
            pltpu.VMEM((ny, 2 * node_count, sc * BINS), f32),
            pltpu.VMEM((ny - 1, 2 * node_count, sc * BINS), f32),
            pltpu.VMEM((2 * node_count, sc * BINS), f32),
            pltpu.VMEM((2 * node_count, sc * BINS), f32),
            pltpu.VMEM((1, LANES), f32),
            pltpu.VMEM((nx * ny * nz - 1, 1, LANES), f32),
            dma((7,)),
            dma((nx - 1,)), dma((nx - 1,)),
            dma((ny, nz)), dma((ny, nz)),
            dma((nz,)), dma((nz,)),
            dma((nz,)), dma((nz,)),
            dma((ny - 1,)), dma((ny - 1,)),
            dma, dma,
            dma, dma,
        ],
        compiler_params=pltpu.CompilerParams(collective_id=0, has_side_effects=True),
        name="level",
    )(split_feature, split_bin, gradients.reshape(shape), hessians.reshape(shape), parents.reshape(shape), elected, binned)
    nodes, best, node_best = pl.pallas_call(
        finish, out_shape=results, in_specs=[vmem] * 3, out_specs=(vmem,) * 3, name="finish"
    )(*outs)
    return nodes.reshape(rows_here), best.T[:, None, :], node_best.reshape(node_count)


def solution(mesh):
    ny, nz, nx = 4, 8, mesh.shape["rep"]
    finer = Mesh(mesh.devices.reshape(ny, nz, 2, nx), ("rows_0", "rows_1", "rows_2", "rep"))
    placed = (P(ROWS, "rep"), P(ROWS), P(ROWS), P(ROWS), P(), P(), P(None, "rep"))
    return jax.shard_map(
        functools.partial(body, (ny, nz, nx)),
        mesh=finer,
        in_specs=placed,
        out_specs=(P(ROWS), P(None, "rep", ROWS), P()),
        check_vma=False,
    )
```

```python
import functools

import jax
import jax.numpy as jnp
from jax import lax
from jax.experimental import pallas as pl
from jax.experimental.pallas import tpu as pltpu
from jax.sharding import Mesh
from jax.sharding import PartitionSpec as P

BINS = 128
LANES = 128
ROWS = ("rows_0", "rows_1", "rows_2")
MESH_IDS = pl.DeviceIdType.MESH
f32, bf16, i32, f8 = jnp.float32, jnp.bfloat16, jnp.int32, jnp.float8_e4m3fn

l2_penalty = 1.0


def iota(shape, dim, dtype=i32):
    out = lax.broadcasted_iota(i32, shape, dim)
    if dtype == bf16:
        return out.astype(f32).astype(bf16)
    return out.astype(dtype)


def remote(src, dst, send, recv, where):
    return pltpu.make_async_remote_copy(
        src_ref=src, dst_ref=dst, send_sem=send, recv_sem=recv, device_id=where, device_id_type=MESH_IDS
    )


def kernel(ny, nz, nx, sc, split_feature_hbm, split_bin_hbm, gradients_hbm, hessians_hbm, parents_hbm, elected_hbm, binned_hbm,
           nodes_out, best_out, node_best_out,
           split_feature, split_bin, gradients, hessians, parents, elected, binned, side, side_in, left_box, outbox, zbox, node_box, stats_box, weights, acc, acc_y, mine, acc_in,
           top, tops,
           answer, load_sems, side_send, side_recv, z_send, z_recv, node_send, node_recv, stats_send, stats_recv,
           y_send, y_recv, core_send, core_recv, top_send, top_recv):
    y, z = lax.axis_index("rows_0"), lax.axis_index("rows_1")
    core, x = lax.axis_index("rows_2"), lax.axis_index("rep")
    parent_count = split_feature.shape[0]
    node_count = elected.shape[0]
    width = binned.shape[1]
    chunks = parents.shape[0]

    def at_x(d):
        return {"rep": lax.rem(x + d, nx)}

    def at_y(d):
        return {"rows_0": lax.rem(y + d, ny)}

    half_z = nz // 2
    side_z, place_z = z // half_z, z % half_z

    def at_z(k):
        other = k // half_z
        base = (side_z + other - 2 * side_z * other) * half_z
        return {"rows_1": base + (place_z + k) % half_z, "rows_2": 1 - core}

    near = [1 + (i // 2 if i % 2 == 0 else half_z - 2 - i // 2) for i in range(half_z - 1)]
    across = [half_z + k for k in ([1 + (i // 2 if i % 2 == 0 else half_z - 2 - i // 2) for i in range(half_z - 1)] + [0])]
    core_mate = {"rows_2": 1 - core}
    beside = [at_x(d) for d in range(1, nx)] + [at_y(d) for d in range(1, ny)] + [core_mate] + [at_z(k) for k in near]
    barrier = pltpu.get_barrier_semaphore()
    for peer in beside:
        pl.semaphore_signal(barrier, inc=1, device_id=peer, device_id_type=MESH_IDS)

    @pl.when(side_z == 0)
    def _():
        for k in across:
            pl.semaphore_signal(barrier, inc=1, device_id=at_z(k), device_id_type=MESH_IDS)

    pairs = ((binned_hbm, binned), (parents_hbm, parents), (split_feature_hbm, split_feature), (split_bin_hbm, split_bin),
             (gradients_hbm, gradients), (hessians_hbm, hessians), (elected_hbm, elected))
    loads = [pltpu.make_async_copy(src, dst, load_sems.at[i]) for i, (src, dst) in enumerate(pairs)]
    for load in loads:
        load.start()

    for load in loads[1:]:
        load.wait()
    stats_box[0, 0] = gradients[...].astype(f32)
    stats_box[0, 1] = hessians[...].astype(f32)
    parent = parents[...].astype(f32)
    parent_rows = iota((parent_count, LANES), 0)
    want = jnp.zeros((parent_count, width), i32)
    bound = jnp.zeros((parent_count, LANES), i32)
    for p in range(parent_count):
        want = jnp.where(iota((parent_count, width), 0) == p, split_feature[p] - x * width, want)
        bound = jnp.where(parent_rows == p, split_bin[p], bound)
    pick = jnp.where(iota((parent_count, width), 1) == want, jnp.ones((), f32), jnp.zeros((), f32)).astype(bf16)
    owned = (want[:, :LANES] >= 0) & (want[:, :LANES] < width)
    loads[0].wait()
    values = lax.dot_general(pick, binned[...].astype(f32).astype(bf16), (((1,), (1,)), ((), ())),
                             preferred_element_type=f32)
    bound = bound.astype(f32)
    for c in range(chunks):
        hit = (parent_rows.astype(f32) == parent[c:c + 1]) & owned & (values[:, c * LANES:(c + 1) * LANES] > bound)
        side[c:c + 1, :] = jnp.max(jnp.where(hit, 1.0, 0.0), axis=0, keepdims=True)

    pl.semaphore_wait(barrier, len(beside) + side_z * len(across))

    @pl.when(side_z == 1)
    def _():
        for k in across:
            pl.semaphore_signal(answer, inc=1, device_id=at_z(k), device_id_type=MESH_IDS)

    side_copies = []
    for d in range(1, nx):
        copy = remote(side, side_in.at[d - 1], side_send.at[d - 1], side_recv.at[d - 1], at_x(d))
        copy.start()
        side_copies.append(copy)
    def stats_to(k):
        return remote(stats_box.at[0], stats_box.at[k], stats_send.at[k], stats_recv.at[k], at_z(k))

    def node_to(k):
        return remote(node_box.at[0], node_box.at[k], node_send.at[k], node_recv.at[k], at_z(k))

    def bins_to(j, k):
        there = lax.rem(y + 1 + j, ny)
        return remote(outbox.at[at_z(k)["rows_1"], there], zbox.at[j, k], z_send.at[j, k], z_recv.at[j, k], at_z(k))

    def send(ks):
        for k in ks:
            node_to(k).start()
        for j in range(ny):
            for k in ks:
                bins_to(j, k).start()

    for k in near:
        stats_to(k).start()

    @pl.when(side_z == 1)
    def _():
        for k in across:
            stats_to(k).start()

    chosen = elected[...].astype(f32).astype(bf16)
    node_rows = iota((node_count, LANES), 0).astype(f32)
    for c in range(chunks):
        rows = slice(c * LANES, (c + 1) * LANES)
        packed = binned[rows, :LANES]
        for b in range(1, width // LANES):
            packed = packed + (binned[rows, b * LANES:(b + 1) * LANES] << (8 * b))
        for way, box in ((0, left_box), (1, outbox)):
            hot = jnp.where(node_rows == 2.0 * parent[c:c + 1] + way, 1.0, 0.0).astype(bf16)
            index = lax.dot_general(hot, chosen, (((0,), (0,)), ((), ())), preferred_element_type=f32).astype(i32)
            found = jnp.take_along_axis(packed, index & (LANES - 1), axis=1, mode="promise_in_bounds")
            found = (found >> ((index >> 7) << 3)) & (BINS - 1)
            turned = found.astype(f32).T
            for yy in range(ny):
                for zz in range(nz):
                    first = (yy * nz + zz) * sc
                    box[zz, yy, :, c, :] = turned[first:first + sc]

    for copy in side_copies:
        copy.wait_recv()
    went = side[...]
    for d in range(1, nx):
        went = went + side_in[d - 1]
    node = 2.0 * parent + went
    nodes_out[...] = node.astype(i32)
    node_box[0] = node
    right = (went > 0.0)[None]
    for yy in range(ny):
        for zz in range(nz):
            outbox[zz, yy] = jnp.where(right, outbox[zz, yy], left_box[zz, yy])
    @pl.when(side_z == 0)
    def _():
        send(near)

    @pl.when(side_z == 1)
    def _():
        send(near + across)

    def weigh(d):
        node_of = iota((node_count, LANES), 0, bf16)
        zero = jnp.zeros((), bf16)
        for c in range(chunks):
            here = node_of == node_box[d, c:c + 1, :].astype(bf16)
            at = slice(c * LANES, (c + 1) * LANES)
            weights[d, :node_count, at] = jnp.where(here, stats_box[d, 0, c:c + 1, :].astype(bf16), zero)
            weights[d, node_count:, at] = jnp.where(here, stats_box[d, 1, c:c + 1, :].astype(bf16), zero)

    def counted(box, d):
        bin_rows = iota((BINS, LANES), 0, bf16)
        one, zero = jnp.ones((), bf16), jnp.zeros((), bf16)
        hots = []
        for s in range(sc):
            row = [box[s, c:c + 1, :].astype(bf16) for c in range(chunks)]
            hots.append(jnp.concatenate([jnp.where(bin_rows == r, one, zero) for r in row], axis=1))
        return lax.dot_general(weights[d], jnp.concatenate(hots, axis=0).astype(f8), (((1,), (1,)), ((), ())),
                               preferred_element_type=f32)

    def wait_for(ref, sem):
        pltpu.make_async_copy(ref, ref, sem).wait()

    weigh(0)

    def own(j, carry):
        acc[j] = counted(outbox.at[z, lax.rem(y + 1 + j, ny)], 0)
        return carry

    lax.fori_loop(0, ny, own, 0)

    @pl.when(side_z == 0)
    def _():
        pl.semaphore_wait(answer, len(across))
        for k in across:
            stats_to(k).start()
        send(across)


    def to_owner(j):
        return remote(acc.at[j], acc_y.at[j], y_send.at[j], y_recv.at[j], at_y(1 + j))

    def add_group(j, group):
        for d in group:
            wait_for(zbox.at[j, d], z_recv.at[j, d])
        acc[j] += functools.reduce(jnp.add, [counted(zbox.at[j, d], d) for d in group])

    ranked = near + across
    cuts = [0, 2, 3, 5, 6, 7] if nz == 8 else list(range(nz))
    late_cuts = [0, 4, 6, 7] if nz == 8 else list(range(nz))
    for lo, hi in zip(cuts, cuts[1:]):
        for d in ranked[lo:hi]:
            wait_for(stats_box.at[d], stats_recv.at[d])
            wait_for(node_box.at[d], node_recv.at[d])
            weigh(d)
        add_group(0, ranked[lo:hi])
    to_owner(0).start()

    def next_round(j, carry):
        for lo, hi in zip(late_cuts, late_cuts[1:]):
            add_group(j, ranked[lo:hi])

        @pl.when(j < ny - 1)
        def _():
            to_owner(j).start()

        return carry

    lax.fori_loop(1, ny, next_round, 0)
    total = acc[ny - 1]
    for j in range(ny - 1):
        to_owner(j).wait_recv()
        total = total + acc_y[j]
    mine[...] = total

    swap = remote(mine, acc_in, core_send, core_recv, core_mate)
    swap.start()
    swap.wait_recv()
    hist = total + acc_in[...]
    upto = jnp.where(iota((BINS, BINS), 0) <= iota((BINS, BINS), 1), 1.0, 0.0)
    lane = iota((node_count, BINS), 1)
    low = jnp.full((), -3.0e38, f32)
    best = []
    for s in range(sc):
        left = jnp.dot(hist[:, s * BINS:(s + 1) * BINS], upto, precision=lax.Precision.HIGHEST,
                       preferred_element_type=f32)
        left_grad, left_hess = left[:node_count], left[node_count:]
        total_grad, total_hess = left_grad[:, BINS - 1:], left_hess[:, BINS - 1:]
        gain = 0.5 * (left_grad * left_grad / (left_hess + l2_penalty)
                      + (total_grad - left_grad) ** 2 / (total_hess - left_hess + l2_penalty)
                      - total_grad * total_grad / (total_hess + l2_penalty))
        best.append(jnp.max(jnp.where(lane < BINS - 1, gain, low), axis=1, keepdims=True))
    half = sc // 2
    diagonal = iota((node_count, LANES), 0) == iota((node_count, LANES), 1)

    def spread(column):
        return jnp.max(jnp.where(diagonal, column, low), axis=0, keepdims=True)

    top[...] = spread(functools.reduce(jnp.maximum, best))
    for s in range(half):
        best_out[s:s + 1] = spread(jnp.where(core == 0, best[s], best[half + s]))[:, :node_count]

    others = [(dx, dy, dz) for dx in range(nx) for dy in range(ny) for dz in range(nz)][1:]
    far = {n: [min(k, n - k) for k in range(n)] for n in (nx, ny, nz)}
    others.sort(key=lambda d: -(far[nx][d[0]] + far[ny][d[1]] + far[nz][d[2]]))
    for i, (dx, dy, dz) in enumerate(others):
        remote(top, tops.at[i], top_send, top_recv,
               {"rep": lax.rem(x + dx, nx), "rows_0": lax.rem(y + dy, ny), "rows_1": lax.rem(z + dz, nz),
                "rows_2": 1 - core}).start()
    wait_for(tops, top_recv)
    node_best_out[...] = jnp.maximum(top[...], jnp.max(tops[...], axis=0))[:, :node_count]

    for copy in side_copies + [swap]:
        copy.wait_send()
    wait_for(tops, top_send)
    for k in range(1, nz):
        stats_to(k).wait_send()
        node_to(k).wait_send()
        for j in range(ny):
            bins_to(j, k).wait_send()
    for j in range(ny - 1):
        to_owner(j).wait_send()


def finish(nodes, best, node_best, nodes_out, best_out, node_best_out, sems):
    pairs = ((nodes, nodes_out), (best, best_out), (node_best, node_best_out))
    copies = [pltpu.make_async_copy(src, dst, sems.at[i]) for i, (src, dst) in enumerate(pairs)]
    for copy in copies:
        copy.start()
    for copy in copies:
        copy.wait()


def body(sizes, binned, gradients, hessians, parents, split_feature, split_bin, elected):
    ny, nz, nx = sizes
    rows_here, width = binned.shape
    node_count, slots_here = elected.shape
    chunks = rows_here // LANES
    sc = slots_here // (ny * nz)
    shape = (chunks, LANES)
    vmem, hbm = pl.BlockSpec(memory_space=pltpu.VMEM), pl.BlockSpec(memory_space=pl.ANY)
    dma = pltpu.SemaphoreType.DMA
    results = (
        jax.ShapeDtypeStruct((chunks, LANES), i32),
        jax.ShapeDtypeStruct((sc // 2, node_count), f32),
        jax.ShapeDtypeStruct((1, node_count), f32),
    )
    outs = pl.pallas_call(
        functools.partial(kernel, ny, nz, nx, sc),
        out_shape=results,
        in_specs=[hbm] * 7,
        out_specs=(vmem, vmem, vmem),
        scratch_shapes=[
            pltpu.SMEM(split_feature.shape, i32),
            pltpu.SMEM(split_bin.shape, i32),
            pltpu.VMEM(shape, bf16),
            pltpu.VMEM(shape, bf16),
            pltpu.VMEM(shape, i32),
            pltpu.VMEM(elected.shape, i32),
            pltpu.VMEM((rows_here, width), i32),
            pltpu.VMEM((chunks, LANES), f32),
            pltpu.VMEM((nx - 1, chunks, LANES), f32),
            pltpu.VMEM((nz, ny, sc, chunks, LANES), f32),
            pltpu.VMEM((nz, ny, sc, chunks, LANES), f32),
            pltpu.VMEM((ny, nz, sc, chunks, LANES), f32),
            pltpu.VMEM((nz, chunks, LANES), f32),
            pltpu.VMEM((nz, 2, chunks, LANES), f32),
            pltpu.VMEM((nz, 2 * node_count, rows_here), bf16),
            pltpu.VMEM((ny, 2 * node_count, sc * BINS), f32),
            pltpu.VMEM((ny - 1, 2 * node_count, sc * BINS), f32),
            pltpu.VMEM((2 * node_count, sc * BINS), f32),
            pltpu.VMEM((2 * node_count, sc * BINS), f32),
            pltpu.VMEM((1, LANES), f32),
            pltpu.VMEM((nx * ny * nz - 1, 1, LANES), f32),
            pltpu.SemaphoreType.REGULAR,
            dma((7,)),
            dma((nx - 1,)), dma((nx - 1,)),
            dma((ny, nz)), dma((ny, nz)),
            dma((nz,)), dma((nz,)),
            dma((nz,)), dma((nz,)),
            dma((ny - 1,)), dma((ny - 1,)),
            dma, dma,
            dma, dma,
        ],
        compiler_params=pltpu.CompilerParams(collective_id=0, has_side_effects=True),
        name="level",
    )(split_feature, split_bin, gradients.reshape(shape), hessians.reshape(shape), parents.reshape(shape), elected, binned)
    nodes, best, node_best = pl.pallas_call(
        finish, out_shape=results, in_specs=[hbm] * 3, out_specs=(hbm,) * 3, scratch_shapes=[dma((3,))], name="finish"
    )(*outs)
    return nodes.reshape(rows_here), best.T[:, None, :], node_best.reshape(node_count)


def solution(mesh):
    ny, nz, nx = 4, 8, mesh.shape["rep"]
    finer = Mesh(mesh.devices.reshape(ny, nz, 2, nx), ("rows_0", "rows_1", "rows_2", "rep"))
    placed = (P(ROWS, "rep"), P(ROWS), P(ROWS), P(ROWS), P(), P(), P(None, "rep"))
    return jax.shard_map(
        functools.partial(body, (ny, nz, nx)),
        mesh=finer,
        in_specs=placed,
        out_specs=(P(ROWS), P(None, "rep", ROWS), P()),
        check_vma=False,
    )
```

```python
import functools

import jax
import jax.numpy as jnp
from jax import lax
from jax.experimental import pallas as pl
from jax.experimental.pallas import tpu as pltpu
from jax.sharding import Mesh
from jax.sharding import PartitionSpec as P

BINS = 128
LANES = 128
ROWS = ("rows_0", "rows_1", "rows_2")
MESH_IDS = pl.DeviceIdType.MESH
f32, bf16, i32, f8 = jnp.float32, jnp.bfloat16, jnp.int32, jnp.float8_e4m3fn

l2_penalty = 1.0


def iota(shape, dim, dtype=i32):
    out = lax.broadcasted_iota(i32, shape, dim)
    if dtype == bf16:
        return out.astype(f32).astype(bf16)
    return out.astype(dtype)


def remote(src, dst, send, recv, where):
    return pltpu.make_async_remote_copy(
        src_ref=src, dst_ref=dst, send_sem=send, recv_sem=recv, device_id=where, device_id_type=MESH_IDS
    )


def kernel(ny, nz, nx, sc, split_feature_hbm, split_bin_hbm, gradients_hbm, hessians_hbm, parents_hbm, elected_hbm, binned_hbm,
           nodes_out, best_out, node_best_out,
           split_feature, split_bin, gradients, hessians, parents, elected, binned, side, side_in, left_box, outbox, zbox, node_box, stats_box, weights, acc, acc_y, mine, acc_in,
           top, tops,
           answer, load_sems, side_send, side_recv, z_send, z_recv, node_send, node_recv, stats_send, stats_recv,
           y_send, y_recv, core_send, core_recv, top_send, top_recv):
    y, z = lax.axis_index("rows_0"), lax.axis_index("rows_1")
    core, x = lax.axis_index("rows_2"), lax.axis_index("rep")
    parent_count = split_feature.shape[0]
    node_count = elected.shape[0]
    width = binned.shape[1]
    chunks = parents.shape[0]

    def at_x(d):
        return {"rep": lax.rem(x + d, nx)}

    def at_y(d):
        return {"rows_0": lax.rem(y + d, ny)}

    def at_z(d):
        return {"rows_1": lax.rem(z + d, nz), "rows_2": 1 - core}

    half_z = nz // 2
    side_z, place_z = z // half_z, z % half_z
    near = [{"rows_1": side_z * half_z + (place_z + k) % half_z, "rows_2": 1 - core} for k in range(1, half_z)]
    across = [{"rows_1": (1 - side_z) * half_z + (place_z + k) % half_z, "rows_2": 1 - core} for k in range(half_z)]
    core_mate = {"rows_2": 1 - core}
    beside = [at_x(d) for d in range(1, nx)] + [at_y(d) for d in range(1, ny)] + [core_mate] + near
    ranked = [(i + 1) // 2 if i % 2 else nz - i // 2 for i in range(1, nz)]
    barrier = pltpu.get_barrier_semaphore()
    for peer in beside:
        pl.semaphore_signal(barrier, inc=1, device_id=peer, device_id_type=MESH_IDS)

    @pl.when(side_z == 0)
    def _():
        for peer in across:
            pl.semaphore_signal(barrier, inc=1, device_id=peer, device_id_type=MESH_IDS)

    pairs = ((binned_hbm, binned), (parents_hbm, parents), (split_feature_hbm, split_feature), (split_bin_hbm, split_bin),
             (gradients_hbm, gradients), (hessians_hbm, hessians), (elected_hbm, elected))
    loads = [pltpu.make_async_copy(src, dst, load_sems.at[i]) for i, (src, dst) in enumerate(pairs)]
    for load in loads:
        load.start()

    for load in loads[1:]:
        load.wait()
    stats_box[0, 0] = gradients[...].astype(f32)
    stats_box[0, 1] = hessians[...].astype(f32)
    parent = parents[...].astype(f32)
    parent_rows = iota((parent_count, LANES), 0)
    want = jnp.zeros((parent_count, width), i32)
    bound = jnp.zeros((parent_count, LANES), i32)
    for p in range(parent_count):
        want = jnp.where(iota((parent_count, width), 0) == p, split_feature[p] - x * width, want)
        bound = jnp.where(parent_rows == p, split_bin[p], bound)
    pick = jnp.where(iota((parent_count, width), 1) == want, jnp.ones((), f32), jnp.zeros((), f32)).astype(bf16)
    owned = (want[:, :LANES] >= 0) & (want[:, :LANES] < width)
    loads[0].wait()
    values = lax.dot_general(pick, binned[...].astype(f32).astype(bf16), (((1,), (1,)), ((), ())),
                             preferred_element_type=f32)
    bound = bound.astype(f32)
    for c in range(chunks):
        hit = (parent_rows.astype(f32) == parent[c:c + 1]) & owned & (values[:, c * LANES:(c + 1) * LANES] > bound)
        side[c:c + 1, :] = jnp.max(jnp.where(hit, 1.0, 0.0), axis=0, keepdims=True)

    pl.semaphore_wait(barrier, len(beside) + side_z * len(across))

    @pl.when(side_z == 1)
    def _():
        for peer in across:
            pl.semaphore_signal(answer, inc=1, device_id=peer, device_id_type=MESH_IDS)

    side_copies = []
    for d in range(1, nx):
        copy = remote(side, side_in.at[d - 1], side_send.at[d - 1], side_recv.at[d - 1], at_x(d))
        copy.start()
        side_copies.append(copy)
    def stats_to(k):
        return remote(stats_box.at[0], stats_box.at[k], stats_send.at[k], stats_recv.at[k], at_z(k))

    def node_to(k):
        return remote(node_box.at[0], node_box.at[k], node_send.at[k], node_recv.at[k], at_z(k))

    def bins_to(j, k):
        there = lax.rem(y + 1 + j, ny)
        return remote(outbox.at[at_z(k)["rows_1"], there], zbox.at[j, k], z_send.at[j, k], z_recv.at[j, k], at_z(k))

    def send_stats():
        for k in ranked:
            stats_to(k).start()

    def send_rows():
        for k in ranked:
            node_to(k).start()
        for j in range(ny):
            for k in ranked:
                bins_to(j, k).start()

    pl.when(side_z == 1)(send_stats)

    chosen = elected[...].astype(f32).astype(bf16)
    node_rows = iota((node_count, LANES), 0).astype(f32)
    for c in range(chunks):
        rows = slice(c * LANES, (c + 1) * LANES)
        packed = binned[rows, :LANES]
        for b in range(1, width // LANES):
            packed = packed + (binned[rows, b * LANES:(b + 1) * LANES] << (8 * b))
        for way, box in ((0, left_box), (1, outbox)):
            hot = jnp.where(node_rows == 2.0 * parent[c:c + 1] + way, 1.0, 0.0).astype(bf16)
            index = lax.dot_general(hot, chosen, (((0,), (0,)), ((), ())), preferred_element_type=f32).astype(i32)
            found = jnp.take_along_axis(packed, index & (LANES - 1), axis=1, mode="promise_in_bounds")
            found = (found >> ((index >> 7) << 3)) & (BINS - 1)
            turned = found.astype(f32).T
            for yy in range(ny):
                for zz in range(nz):
                    first = (yy * nz + zz) * sc
                    box[zz, yy, :, c, :] = turned[first:first + sc]

    for copy in side_copies:
        copy.wait_recv()
    went = side[...]
    for d in range(1, nx):
        went = went + side_in[d - 1]
    node = 2.0 * parent + went
    nodes_out[...] = node.astype(i32)
    node_box[0] = node
    right = (went > 0.0)[None]
    for yy in range(ny):
        for zz in range(nz):
            outbox[zz, yy] = jnp.where(right, outbox[zz, yy], left_box[zz, yy])
    pl.when(side_z == 1)(send_rows)

    def weigh(d):
        node_of = iota((node_count, LANES), 0, bf16)
        zero = jnp.zeros((), bf16)
        for c in range(chunks):
            here = node_of == node_box[d, c:c + 1, :].astype(bf16)
            at = slice(c * LANES, (c + 1) * LANES)
            weights[d, :node_count, at] = jnp.where(here, stats_box[d, 0, c:c + 1, :].astype(bf16), zero)
            weights[d, node_count:, at] = jnp.where(here, stats_box[d, 1, c:c + 1, :].astype(bf16), zero)

    def counted(box, d):
        bin_rows = iota((BINS, LANES), 0, bf16)
        one, zero = jnp.ones((), bf16), jnp.zeros((), bf16)
        hots = []
        for s in range(sc):
            row = [box[s, c:c + 1, :].astype(bf16) for c in range(chunks)]
            hots.append(jnp.concatenate([jnp.where(bin_rows == r, one, zero) for r in row], axis=1))
        return lax.dot_general(weights[d], jnp.concatenate(hots, axis=0).astype(f8), (((1,), (1,)), ((), ())),
                               preferred_element_type=f32)

    def wait_for(ref, sem):
        pltpu.make_async_copy(ref, ref, sem).wait()

    weigh(0)

    def own(j, carry):
        acc[j] = counted(outbox.at[z, lax.rem(y + 1 + j, ny)], 0)
        return carry

    lax.fori_loop(0, ny, own, 0)

    @pl.when(side_z == 0)
    def _():
        pl.semaphore_wait(answer, len(across))
        send_stats()
        send_rows()

    def to_owner(j):
        return remote(acc.at[j], acc_y.at[j], y_send.at[j], y_recv.at[j], at_y(1 + j))

    def add_group(j, group):
        for d in group:
            wait_for(zbox.at[j, d], z_recv.at[j, d])
        acc[j] += functools.reduce(jnp.add, [counted(zbox.at[j, d], d) for d in group])

    cuts = list(range(0, nz - 1, 2)) + [nz - 1]
    late_cuts = [0, 4, 6, 7] if nz == 8 else cuts
    for lo, hi in zip(cuts, cuts[1:]):
        for d in ranked[lo:hi]:
            wait_for(stats_box.at[d], stats_recv.at[d])
            wait_for(node_box.at[d], node_recv.at[d])
            weigh(d)
        add_group(0, ranked[lo:hi])
    to_owner(0).start()

    def next_round(j, carry):
        for lo, hi in zip(late_cuts, late_cuts[1:]):
            add_group(j, ranked[lo:hi])

        @pl.when(j < ny - 1)
        def _():
            to_owner(j).start()

        return carry

    lax.fori_loop(1, ny, next_round, 0)
    total = acc[ny - 1]
    for j in range(ny - 1):
        to_owner(j).wait_recv()
        total = total + acc_y[j]
    mine[...] = total

    swap = remote(mine, acc_in, core_send, core_recv, core_mate)
    swap.start()
    swap.wait_recv()
    hist = total + acc_in[...]
    upto = jnp.where(iota((BINS, BINS), 0) <= iota((BINS, BINS), 1), 1.0, 0.0)
    lane = iota((node_count, BINS), 1)
    low = jnp.full((), -3.0e38, f32)
    best = []
    for s in range(sc):
        left = jnp.dot(hist[:, s * BINS:(s + 1) * BINS], upto, precision=lax.Precision.HIGHEST,
                       preferred_element_type=f32)
        left_grad, left_hess = left[:node_count], left[node_count:]
        total_grad, total_hess = left_grad[:, BINS - 1:], left_hess[:, BINS - 1:]
        gain = 0.5 * (left_grad * left_grad / (left_hess + l2_penalty)
                      + (total_grad - left_grad) ** 2 / (total_hess - left_hess + l2_penalty)
                      - total_grad * total_grad / (total_hess + l2_penalty))
        best.append(jnp.max(jnp.where(lane < BINS - 1, gain, low), axis=1, keepdims=True))
    half = sc // 2
    diagonal = iota((node_count, LANES), 0) == iota((node_count, LANES), 1)

    def spread(column):
        return jnp.max(jnp.where(diagonal, column, low), axis=0, keepdims=True)

    top[...] = spread(functools.reduce(jnp.maximum, best))
    for s in range(half):
        best_out[s:s + 1] = spread(jnp.where(core == 0, best[s], best[half + s]))[:, :node_count]

    others = [(dx, dy, dz) for dx in range(nx) for dy in range(ny) for dz in range(nz)][1:]
    far = {n: [min(k, n - k) for k in range(n)] for n in (nx, ny, nz)}
    others.sort(key=lambda d: -(far[nx][d[0]] + far[ny][d[1]] + far[nz][d[2]]))
    for i, (dx, dy, dz) in enumerate(others):
        remote(top, tops.at[i], top_send, top_recv,
               {"rep": lax.rem(x + dx, nx), "rows_0": lax.rem(y + dy, ny), "rows_1": lax.rem(z + dz, nz),
                "rows_2": 1 - core}).start()
    wait_for(tops, top_recv)
    node_best_out[...] = jnp.maximum(top[...], jnp.max(tops[...], axis=0))[:, :node_count]

    for copy in side_copies + [swap]:
        copy.wait_send()
    wait_for(tops, top_send)
    for k in range(1, nz):
        stats_to(k).wait_send()
        node_to(k).wait_send()
        for j in range(ny):
            bins_to(j, k).wait_send()
    for j in range(ny - 1):
        to_owner(j).wait_send()


def finish(nodes, best, node_best, nodes_out, best_out, node_best_out):
    nodes_out[...] = nodes[...]
    best_out[...] = best[...]
    node_best_out[...] = node_best[...]


def body(sizes, binned, gradients, hessians, parents, split_feature, split_bin, elected):
    ny, nz, nx = sizes
    rows_here, width = binned.shape
    node_count, slots_here = elected.shape
    chunks = rows_here // LANES
    sc = slots_here // (ny * nz)
    shape = (chunks, LANES)
    vmem, hbm = pl.BlockSpec(memory_space=pltpu.VMEM), pl.BlockSpec(memory_space=pl.ANY)
    dma = pltpu.SemaphoreType.DMA
    results = (
        jax.ShapeDtypeStruct((chunks, LANES), i32),
        jax.ShapeDtypeStruct((sc // 2, node_count), f32),
        jax.ShapeDtypeStruct((1, node_count), f32),
    )
    outs = pl.pallas_call(
        functools.partial(kernel, ny, nz, nx, sc),
        out_shape=tuple(pltpu.VMEM(r.shape, r.dtype) for r in results),
        in_specs=[hbm] * 7,
        out_specs=(vmem, vmem, vmem),
        scratch_shapes=[
            pltpu.SMEM(split_feature.shape, i32),
            pltpu.SMEM(split_bin.shape, i32),
            pltpu.VMEM(shape, bf16),
            pltpu.VMEM(shape, bf16),
            pltpu.VMEM(shape, i32),
            pltpu.VMEM(elected.shape, i32),
            pltpu.VMEM((rows_here, width), i32),
            pltpu.VMEM((chunks, LANES), f32),
            pltpu.VMEM((nx - 1, chunks, LANES), f32),
            pltpu.VMEM((nz, ny, sc, chunks, LANES), f32),
            pltpu.VMEM((nz, ny, sc, chunks, LANES), f32),
            pltpu.VMEM((ny, nz, sc, chunks, LANES), f32),
            pltpu.VMEM((nz, chunks, LANES), f32),
            pltpu.VMEM((nz, 2, chunks, LANES), f32),
            pltpu.VMEM((nz, 2 * node_count, rows_here), bf16),
            pltpu.VMEM((ny, 2 * node_count, sc * BINS), f32),
            pltpu.VMEM((ny - 1, 2 * node_count, sc * BINS), f32),
            pltpu.VMEM((2 * node_count, sc * BINS), f32),
            pltpu.VMEM((2 * node_count, sc * BINS), f32),
            pltpu.VMEM((1, LANES), f32),
            pltpu.VMEM((nx * ny * nz - 1, 1, LANES), f32),
            pltpu.SemaphoreType.REGULAR,
            dma((7,)),
            dma((nx - 1,)), dma((nx - 1,)),
            dma((ny, nz)), dma((ny, nz)),
            dma((nz,)), dma((nz,)),
            dma((nz,)), dma((nz,)),
            dma((ny - 1,)), dma((ny - 1,)),
            dma, dma,
            dma, dma,
        ],
        compiler_params=pltpu.CompilerParams(collective_id=0, has_side_effects=True),
        name="level",
    )(split_feature, split_bin, gradients.reshape(shape), hessians.reshape(shape), parents.reshape(shape), elected, binned)
    nodes, best, node_best = pl.pallas_call(
        finish, out_shape=results, in_specs=[vmem] * 3, out_specs=(vmem,) * 3, name="finish"
    )(*(pltpu.with_memory_space_constraint(out, pltpu.VMEM) for out in outs))
    return nodes.reshape(rows_here), best.T[:, None, :], node_best.reshape(node_count)


def solution(mesh):
    ny, nz, nx = 4, 8, mesh.shape["rep"]
    finer = Mesh(mesh.devices.reshape(ny, nz, 2, nx), ("rows_0", "rows_1", "rows_2", "rep"))
    placed = (P(ROWS, "rep"), P(ROWS), P(ROWS), P(ROWS), P(), P(), P(None, "rep"))
    return jax.shard_map(
        functools.partial(body, (ny, nz, nx)),
        mesh=finer,
        in_specs=placed,
        out_specs=(P(ROWS), P(None, "rep", ROWS), P()),
        check_vma=False,
    )
```

```python
import functools

import jax
import jax.numpy as jnp
from jax import lax
from jax.experimental import pallas as pl
from jax.experimental.pallas import tpu as pltpu
from jax.sharding import Mesh
from jax.sharding import PartitionSpec as P

BINS = 128
LANES = 128
ROWS = ("rows_0", "rows_1", "rows_2")
MESH_IDS = pl.DeviceIdType.MESH
f32, bf16, i32, f8 = jnp.float32, jnp.bfloat16, jnp.int32, jnp.float8_e4m3fn

l2_penalty = 1.0


def iota(shape, dim, dtype=i32):
    out = lax.broadcasted_iota(i32, shape, dim)
    if dtype == bf16:
        return out.astype(f32).astype(bf16)
    return out.astype(dtype)


def remote(src, dst, send, recv, where):
    return pltpu.make_async_remote_copy(
        src_ref=src, dst_ref=dst, send_sem=send, recv_sem=recv, device_id=where, device_id_type=MESH_IDS
    )


def kernel(ny, nz, nx, sc, split_feature_hbm, split_bin_hbm, gradients_hbm, hessians_hbm, parents_hbm, elected_hbm, binned_hbm,
           nodes_out, best_out, node_best_out,
           split_feature, split_bin, gradients, hessians, parents, elected, binned, side, side_in, left_box, outbox, zbox, node_box, stats_box, weights, acc, acc_y, mine, acc_in,
           top, tops,
           load_sems, side_send, side_recv, z_send, z_recv, node_send, node_recv, stats_send, stats_recv,
           y_send, y_recv, core_send, core_recv, top_send, top_recv):
    y, z = lax.axis_index("rows_0"), lax.axis_index("rows_1")
    core, x = lax.axis_index("rows_2"), lax.axis_index("rep")
    parent_count = split_feature.shape[0]
    node_count = elected.shape[0]
    width = binned.shape[1]
    chunks = parents.shape[0]

    def at_x(d):
        return {"rep": lax.rem(x + d, nx)}

    def at_y(d):
        return {"rows_0": lax.rem(y + d, ny)}

    def at_z(d):
        return {"rows_1": lax.rem(z + d, nz), "rows_2": 1 - core}

    core_mate = {"rows_2": 1 - core}
    beside = [at_x(d) for d in range(1, nx)] + [at_y(d) for d in range(1, ny)] + [core_mate] + [at_z(d) for d in range(1, nz)]
    ranked = [4, 1, 7, 3, 5, 2, 6] if nz == 8 else list(range(1, nz))
    barrier = pltpu.get_barrier_semaphore()
    for peer in beside:
        pl.semaphore_signal(barrier, inc=1, device_id=peer, device_id_type=MESH_IDS)

    pairs = ((binned_hbm, binned), (parents_hbm, parents), (split_feature_hbm, split_feature), (split_bin_hbm, split_bin),
             (gradients_hbm, gradients), (hessians_hbm, hessians), (elected_hbm, elected))
    loads = [pltpu.make_async_copy(src, dst, load_sems.at[i]) for i, (src, dst) in enumerate(pairs)]
    for load in loads:
        load.start()

    for load in loads[1:]:
        load.wait()
    stats_box[0, 0] = gradients[...].astype(f32)
    stats_box[0, 1] = hessians[...].astype(f32)
    parent = parents[...].astype(f32)
    parent_rows = iota((parent_count, LANES), 0)
    want = jnp.zeros((parent_count, width), i32)
    bound = jnp.zeros((parent_count, LANES), i32)
    for p in range(parent_count):
        want = jnp.where(iota((parent_count, width), 0) == p, split_feature[p] - x * width, want)
        bound = jnp.where(parent_rows == p, split_bin[p], bound)
    pick = jnp.where(iota((parent_count, width), 1) == want, jnp.ones((), f32), jnp.zeros((), f32)).astype(bf16)
    owned = (want[:, :LANES] >= 0) & (want[:, :LANES] < width)
    loads[0].wait()
    values = lax.dot_general(pick, binned[...].astype(f32).astype(bf16), (((1,), (1,)), ((), ())),
                             preferred_element_type=f32)
    bound = bound.astype(f32)
    for c in range(chunks):
        hit = (parent_rows.astype(f32) == parent[c:c + 1]) & owned & (values[:, c * LANES:(c + 1) * LANES] > bound)
        side[c:c + 1, :] = jnp.max(jnp.where(hit, 1.0, 0.0), axis=0, keepdims=True)

    pl.semaphore_wait(barrier, len(beside))
    side_copies = []
    for d in range(1, nx):
        copy = remote(side, side_in.at[d - 1], side_send.at[d - 1], side_recv.at[d - 1], at_x(d))
        copy.start()
        side_copies.append(copy)
    def stats_to(k):
        return remote(stats_box.at[0], stats_box.at[k], stats_send.at[k], stats_recv.at[k], at_z(k))

    def node_to(k):
        return remote(node_box.at[0], node_box.at[k], node_send.at[k], node_recv.at[k], at_z(k))

    def bins_to(j, k):
        there = lax.rem(y + 1 + j, ny)
        return remote(outbox.at[at_z(k)["rows_1"], there], zbox.at[j, k], z_send.at[j, k], z_recv.at[j, k], at_z(k))

    def send_stats():
        for k in ranked:
            stats_to(k).start()

    def send_rows():
        for k in ranked:
            node_to(k).start()
        for j in range(ny):
            for k in ranked:
                bins_to(j, k).start()

    send_stats()

    chosen = elected[...].astype(f32).astype(bf16)
    node_rows = iota((node_count, LANES), 0).astype(f32)
    for c in range(chunks):
        rows = slice(c * LANES, (c + 1) * LANES)
        packed = binned[rows, :LANES]
        for b in range(1, width // LANES):
            packed = packed + (binned[rows, b * LANES:(b + 1) * LANES] << (8 * b))
        for way, box in ((0, left_box), (1, outbox)):
            hot = jnp.where(node_rows == 2.0 * parent[c:c + 1] + way, 1.0, 0.0).astype(bf16)
            index = lax.dot_general(hot, chosen, (((0,), (0,)), ((), ())), preferred_element_type=f32).astype(i32)
            found = jnp.take_along_axis(packed, index & (LANES - 1), axis=1, mode="promise_in_bounds")
            found = (found >> ((index >> 7) << 3)) & (BINS - 1)
            turned = found.astype(f32).T
            for yy in range(ny):
                for zz in range(nz):
                    first = (yy * nz + zz) * sc
                    box[zz, yy, :, c, :] = turned[first:first + sc]

    for copy in side_copies:
        copy.wait_recv()
    went = side[...]
    for d in range(1, nx):
        went = went + side_in[d - 1]
    node = 2.0 * parent + went
    nodes_out[...] = node.astype(i32)
    node_box[0] = node
    right = (went > 0.0)[None]
    for yy in range(ny):
        for zz in range(nz):
            outbox[zz, yy] = jnp.where(right, outbox[zz, yy], left_box[zz, yy])
    send_rows()

    def weigh(d):
        node_of = iota((node_count, LANES), 0, bf16)
        zero = jnp.zeros((), bf16)
        for c in range(chunks):
            here = node_of == node_box[d, c:c + 1, :].astype(bf16)
            at = slice(c * LANES, (c + 1) * LANES)
            weights[d, :node_count, at] = jnp.where(here, stats_box[d, 0, c:c + 1, :].astype(bf16), zero)
            weights[d, node_count:, at] = jnp.where(here, stats_box[d, 1, c:c + 1, :].astype(bf16), zero)

    def counted(box, d):
        bin_rows = iota((BINS, LANES), 0, bf16)
        one, zero = jnp.ones((), bf16), jnp.zeros((), bf16)
        hots = []
        for s in range(sc):
            row = [box[s, c:c + 1, :].astype(bf16) for c in range(chunks)]
            hots.append(jnp.concatenate([jnp.where(bin_rows == r, one, zero) for r in row], axis=1))
        return lax.dot_general(weights[d], jnp.concatenate(hots, axis=0).astype(f8), (((1,), (1,)), ((), ())),
                               preferred_element_type=f32)

    def wait_for(ref, sem):
        pltpu.make_async_copy(ref, ref, sem).wait()

    weigh(0)

    def own(j, carry):
        acc[j] = counted(outbox.at[z, lax.rem(y + 1 + j, ny)], 0)
        return carry

    lax.fori_loop(0, ny, own, 0)
    def to_owner(j):
        return remote(acc.at[j], acc_y.at[j], y_send.at[j], y_recv.at[j], at_y(1 + j))

    def add_group(j, group):
        for d in group:
            wait_for(zbox.at[j, d], z_recv.at[j, d])
        acc[j] += functools.reduce(jnp.add, [counted(zbox.at[j, d], d) for d in group])

    cuts = list(range(0, nz - 1, 2)) + [nz - 1]
    late_cuts = [0, 4, 6, 7] if nz == 8 else cuts
    for lo, hi in zip(cuts, cuts[1:]):
        for d in ranked[lo:hi]:
            wait_for(stats_box.at[d], stats_recv.at[d])
            wait_for(node_box.at[d], node_recv.at[d])
            weigh(d)
        add_group(0, ranked[lo:hi])
    to_owner(0).start()

    def next_round(j, carry):
        for lo, hi in zip(late_cuts, late_cuts[1:]):
            add_group(j, ranked[lo:hi])

        @pl.when(j < ny - 1)
        def _():
            to_owner(j).start()

        return carry

    lax.fori_loop(1, ny, next_round, 0)
    total = acc[ny - 1]
    for j in range(ny - 1):
        to_owner(j).wait_recv()
        total = total + acc_y[j]
    mine[...] = total

    swap = remote(mine, acc_in, core_send, core_recv, core_mate)
    swap.start()
    swap.wait_recv()
    hist = total + acc_in[...]
    upto = jnp.where(iota((BINS, BINS), 0) <= iota((BINS, BINS), 1), 1.0, 0.0)
    lane = iota((node_count, BINS), 1)
    low = jnp.full((), -3.0e38, f32)
    best = []
    for s in range(sc):
        left = jnp.dot(hist[:, s * BINS:(s + 1) * BINS], upto, precision=lax.Precision.HIGHEST,
                       preferred_element_type=f32)
        left_grad, left_hess = left[:node_count], left[node_count:]
        total_grad, total_hess = left_grad[:, BINS - 1:], left_hess[:, BINS - 1:]
        gain = 0.5 * (left_grad * left_grad / (left_hess + l2_penalty)
                      + (total_grad - left_grad) ** 2 / (total_hess - left_hess + l2_penalty)
                      - total_grad * total_grad / (total_hess + l2_penalty))
        best.append(jnp.max(jnp.where(lane < BINS - 1, gain, low), axis=1, keepdims=True))
    half = sc // 2
    diagonal = iota((node_count, LANES), 0) == iota((node_count, LANES), 1)

    def spread(column):
        return jnp.max(jnp.where(diagonal, column, low), axis=0, keepdims=True)

    top[...] = spread(functools.reduce(jnp.maximum, best))
    for s in range(half):
        best_out[s:s + 1] = spread(jnp.where(core == 0, best[s], best[half + s]))[:, :node_count]

    others = [(dx, dy, dz) for dx in range(nx) for dy in range(ny) for dz in range(nz)][1:]
    far = {n: [min(k, n - k) for k in range(n)] for n in (nx, ny, nz)}
    others.sort(key=lambda d: -(far[nx][d[0]] + far[ny][d[1]] + far[nz][d[2]]))
    for i, (dx, dy, dz) in enumerate(others):
        remote(top, tops.at[i], top_send, top_recv,
               {"rep": lax.rem(x + dx, nx), "rows_0": lax.rem(y + dy, ny), "rows_1": lax.rem(z + dz, nz),
                "rows_2": 1 - core}).start()
    wait_for(tops, top_recv)
    node_best_out[...] = jnp.maximum(top[...], jnp.max(tops[...], axis=0))[:, :node_count]

    for copy in side_copies + [swap]:
        copy.wait_send()
    wait_for(tops, top_send)
    for k in range(1, nz):
        stats_to(k).wait_send()
        node_to(k).wait_send()
        for j in range(ny):
            bins_to(j, k).wait_send()
    for j in range(ny - 1):
        to_owner(j).wait_send()


def finish(nodes, best, node_best, nodes_out, best_out, node_best_out):
    nodes_out[...] = nodes[...]
    best_out[...] = best[...]
    node_best_out[...] = node_best[...]


def body(sizes, binned, gradients, hessians, parents, split_feature, split_bin, elected):
    ny, nz, nx = sizes
    rows_here, width = binned.shape
    node_count, slots_here = elected.shape
    chunks = rows_here // LANES
    sc = slots_here // (ny * nz)
    shape = (chunks, LANES)
    vmem, hbm = pl.BlockSpec(memory_space=pltpu.VMEM), pl.BlockSpec(memory_space=pl.ANY)
    dma = pltpu.SemaphoreType.DMA
    results = (
        jax.ShapeDtypeStruct((chunks, LANES), i32),
        jax.ShapeDtypeStruct((sc // 2, node_count), f32),
        jax.ShapeDtypeStruct((1, node_count), f32),
    )
    outs = pl.pallas_call(
        functools.partial(kernel, ny, nz, nx, sc),
        out_shape=tuple(pltpu.VMEM(r.shape, r.dtype) for r in results),
        in_specs=[hbm] * 7,
        out_specs=(vmem, vmem, vmem),
        scratch_shapes=[
            pltpu.SMEM(split_feature.shape, i32),
            pltpu.SMEM(split_bin.shape, i32),
            pltpu.VMEM(shape, bf16),
            pltpu.VMEM(shape, bf16),
            pltpu.VMEM(shape, i32),
            pltpu.VMEM(elected.shape, i32),
            pltpu.VMEM((rows_here, width), i32),
            pltpu.VMEM((chunks, LANES), f32),
            pltpu.VMEM((nx - 1, chunks, LANES), f32),
            pltpu.VMEM((nz, ny, sc, chunks, LANES), f32),
            pltpu.VMEM((nz, ny, sc, chunks, LANES), f32),
            pltpu.VMEM((ny, nz, sc, chunks, LANES), f32),
            pltpu.VMEM((nz, chunks, LANES), f32),
            pltpu.VMEM((nz, 2, chunks, LANES), f32),
            pltpu.VMEM((nz, 2 * node_count, rows_here), bf16),
            pltpu.VMEM((ny, 2 * node_count, sc * BINS), f32),
            pltpu.VMEM((ny - 1, 2 * node_count, sc * BINS), f32),
            pltpu.VMEM((2 * node_count, sc * BINS), f32),
            pltpu.VMEM((2 * node_count, sc * BINS), f32),
            pltpu.VMEM((1, LANES), f32),
            pltpu.VMEM((nx * ny * nz - 1, 1, LANES), f32),
            dma((7,)),
            dma((nx - 1,)), dma((nx - 1,)),
            dma((ny, nz)), dma((ny, nz)),
            dma((nz,)), dma((nz,)),
            dma((nz,)), dma((nz,)),
            dma((ny - 1,)), dma((ny - 1,)),
            dma, dma,
            dma, dma,
        ],
        compiler_params=pltpu.CompilerParams(collective_id=0, has_side_effects=True),
        name="level",
    )(split_feature, split_bin, gradients.reshape(shape), hessians.reshape(shape), parents.reshape(shape), elected, binned)
    nodes, best, node_best = pl.pallas_call(
        finish, out_shape=results, in_specs=[vmem] * 3, out_specs=(vmem,) * 3, name="finish"
    )(*(pltpu.with_memory_space_constraint(out, pltpu.VMEM) for out in outs))
    return nodes.reshape(rows_here), best.T[:, None, :], node_best.reshape(node_count)


def solution(mesh):
    ny, nz, nx = 4, 8, mesh.shape["rep"]
    finer = Mesh(mesh.devices.reshape(ny, nz, 2, nx), ("rows_0", "rows_1", "rows_2", "rep"))
    placed = (P(ROWS, "rep"), P(ROWS), P(ROWS), P(ROWS), P(), P(), P(None, "rep"))
    return jax.shard_map(
        functools.partial(body, (ny, nz, nx)),
        mesh=finer,
        in_specs=placed,
        out_specs=(P(ROWS), P(None, "rep", ROWS), P()),
        check_vma=False,
    )
```

```python
import functools

import jax
import jax.numpy as jnp
from jax import lax
from jax.experimental import pallas as pl
from jax.experimental.pallas import tpu as pltpu
from jax.sharding import Mesh
from jax.sharding import PartitionSpec as P

BINS = 128
LANES = 128
ROWS = ("rows_0", "rows_1", "rows_2")
MESH_IDS = pl.DeviceIdType.MESH
f32, bf16, i32, f8 = jnp.float32, jnp.bfloat16, jnp.int32, jnp.float8_e4m3fn

l2_penalty = 1.0


def iota(shape, dim, dtype=i32):
    out = lax.broadcasted_iota(i32, shape, dim)
    if dtype == bf16:
        return out.astype(f32).astype(bf16)
    return out.astype(dtype)


def remote(src, dst, send, recv, where):
    return pltpu.make_async_remote_copy(
        src_ref=src, dst_ref=dst, send_sem=send, recv_sem=recv, device_id=where, device_id_type=MESH_IDS
    )


def kernel(ny, nz, nx, sc, split_feature_hbm, split_bin_hbm, gradients_hbm, hessians_hbm, parents_hbm, elected_hbm, binned_hbm,
           nodes_out, best_out, node_best_out,
           split_feature, split_bin, gradients, hessians, parents, elected, binned, side, side_in, left_box, outbox, zbox, node_box, stats_box, weights, acc, acc_y, mine, acc_in,
           top, tops,
           load_sems, side_send, side_recv, z_send, z_recv, node_send, node_recv, stats_send, stats_recv,
           y_send, y_recv, core_send, core_recv, top_send, top_recv):
    y, z = lax.axis_index("rows_0"), lax.axis_index("rows_1")
    core, x = lax.axis_index("rows_2"), lax.axis_index("rep")
    parent_count = split_feature.shape[0]
    node_count = elected.shape[0]
    width = binned.shape[1]
    chunks = parents.shape[0]

    def at_x(d):
        return {"rep": lax.rem(x + d, nx)}

    def at_y(d):
        return {"rows_0": lax.rem(y + d, ny)}

    def at_z(d):
        return {"rows_1": lax.rem(z + d, nz), "rows_2": 1 - core}

    core_mate = {"rows_2": 1 - core}
    beside = [at_x(d) for d in range(1, nx)] + [at_y(d) for d in range(1, ny)] + [core_mate] + [at_z(d) for d in range(1, nz)]
    ranked = [4, 3, 5, 2, 6, 1, 7] if nz == 8 else list(range(1, nz))
    barrier = pltpu.get_barrier_semaphore()
    for peer in beside:
        pl.semaphore_signal(barrier, inc=1, device_id=peer, device_id_type=MESH_IDS)

    pairs = ((binned_hbm, binned), (parents_hbm, parents), (split_feature_hbm, split_feature), (split_bin_hbm, split_bin),
             (gradients_hbm, gradients), (hessians_hbm, hessians), (elected_hbm, elected))
    loads = [pltpu.make_async_copy(src, dst, load_sems.at[i]) for i, (src, dst) in enumerate(pairs)]
    for load in loads:
        load.start()

    for load in loads[1:]:
        load.wait()
    stats_box[0, 0] = gradients[...].astype(f32)
    stats_box[0, 1] = hessians[...].astype(f32)
    parent = parents[...].astype(f32)
    parent_rows = iota((parent_count, LANES), 0)
    want = jnp.zeros((parent_count, width), i32)
    bound = jnp.zeros((parent_count, LANES), i32)
    for p in range(parent_count):
        want = jnp.where(iota((parent_count, width), 0) == p, split_feature[p] - x * width, want)
        bound = jnp.where(parent_rows == p, split_bin[p], bound)
    pick = jnp.where(iota((parent_count, width), 1) == want, jnp.ones((), f32), jnp.zeros((), f32)).astype(bf16)
    owned = (want[:, :LANES] >= 0) & (want[:, :LANES] < width)
    loads[0].wait()
    values = lax.dot_general(pick, binned[...].astype(f32).astype(bf16), (((1,), (1,)), ((), ())),
                             preferred_element_type=f32)
    bound = bound.astype(f32)
    for c in range(chunks):
        hit = (parent_rows.astype(f32) == parent[c:c + 1]) & owned & (values[:, c * LANES:(c + 1) * LANES] > bound)
        side[c:c + 1, :] = jnp.max(jnp.where(hit, 1.0, 0.0), axis=0, keepdims=True)

    pl.semaphore_wait(barrier, len(beside))
    side_copies = []
    for d in range(1, nx):
        copy = remote(side, side_in.at[d - 1], side_send.at[d - 1], side_recv.at[d - 1], at_x(d))
        copy.start()
        side_copies.append(copy)
    def stats_to(k):
        return remote(stats_box.at[0], stats_box.at[k], stats_send.at[k], stats_recv.at[k], at_z(k))

    def node_to(k):
        return remote(node_box.at[0], node_box.at[k], node_send.at[k], node_recv.at[k], at_z(k))

    part = sc // 2

    def bins_to(h, k):
        there, lo = lax.rem(y + 1 + h // 2, ny), h % 2 * part
        return remote(outbox.at[lax.rem(z + k, nz), there, pl.ds(lo, part)], zbox.at[h, k],
                      z_send.at[h, k], z_recv.at[h, k], at_z(k))

    def send_stats():
        for k in ranked:
            stats_to(k).start()

    def send_rows():
        for k in ranked:
            node_to(k).start()
        for h in range(2 * ny):
            for k in ranked:
                bins_to(h, k).start()

    send_stats()

    chosen = elected[...].astype(f32).astype(bf16)
    node_rows = iota((node_count, LANES), 0).astype(f32)
    for c in range(chunks):
        rows = slice(c * LANES, (c + 1) * LANES)
        packed = binned[rows, :LANES]
        for b in range(1, width // LANES):
            packed = packed + (binned[rows, b * LANES:(b + 1) * LANES] << (8 * b))
        for way, box in ((0, left_box), (1, outbox)):
            hot = jnp.where(node_rows == 2.0 * parent[c:c + 1] + way, 1.0, 0.0).astype(bf16)
            index = lax.dot_general(hot, chosen, (((0,), (0,)), ((), ())), preferred_element_type=f32).astype(i32)
            found = jnp.take_along_axis(packed, index & (LANES - 1), axis=1, mode="promise_in_bounds")
            found = (found >> ((index >> 7) << 3)) & (BINS - 1)
            turned = found.astype(f32).T
            for yy in range(ny):
                for zz in range(nz):
                    first = (yy * nz + zz) * sc
                    box[zz, yy, :, c, :] = turned[first:first + sc]

    for copy in side_copies:
        copy.wait_recv()
    went = side[...]
    for d in range(1, nx):
        went = went + side_in[d - 1]
    node = 2.0 * parent + went
    nodes_out[...] = node.astype(i32)
    node_box[0] = node
    right = (went > 0.0)[None]
    for yy in range(ny):
        for zz in range(nz):
            outbox[zz, yy] = jnp.where(right, outbox[zz, yy], left_box[zz, yy])
    send_rows()

    def weigh(d):
        node_of = iota((node_count, LANES), 0, bf16)
        zero = jnp.zeros((), bf16)
        for c in range(chunks):
            here = node_of == node_box[d, c:c + 1, :].astype(bf16)
            at = slice(c * LANES, (c + 1) * LANES)
            weights[d, :node_count, at] = jnp.where(here, stats_box[d, 0, c:c + 1, :].astype(bf16), zero)
            weights[d, node_count:, at] = jnp.where(here, stats_box[d, 1, c:c + 1, :].astype(bf16), zero)

    def counted(box, d):
        bin_rows = iota((BINS, LANES), 0, bf16)
        one, zero = jnp.ones((), bf16), jnp.zeros((), bf16)
        hots = []
        for s in range(part):
            row = [box[s, c:c + 1, :].astype(bf16) for c in range(chunks)]
            hots.append(jnp.concatenate([jnp.where(bin_rows == r, one, zero) for r in row], axis=1))
        return lax.dot_general(weights[d], jnp.concatenate(hots, axis=0).astype(f8), (((1,), (1,)), ((), ())),
                               preferred_element_type=f32)

    def wait_for(ref, sem):
        pltpu.make_async_copy(ref, ref, sem).wait()

    weigh(0)

    def own(h, carry):
        acc[h] = counted(outbox.at[z, lax.rem(y + 1 + h // 2, ny), pl.ds(h % 2 * part, part)], 0)
        return carry

    lax.fori_loop(0, 2 * ny, own, 0)
    def to_owner(h):
        return remote(acc.at[h], acc_y.at[h], y_send.at[h], y_recv.at[h], at_y(1 + h // 2))

    def add_group(h, group):
        for d in group:
            wait_for(zbox.at[h, d], z_recv.at[h, d])
        acc[h] += functools.reduce(jnp.add, [counted(zbox.at[h, d], d) for d in group])

    cuts, later = ([0, 2, 4, 6, 7], [0, 7]) if nz == 8 else ([0, nz - 1],) * 2
    for lo, hi in zip(cuts, cuts[1:]):
        for d in ranked[lo:hi]:
            wait_for(stats_box.at[d], stats_recv.at[d])
            wait_for(node_box.at[d], node_recv.at[d])
            weigh(d)
        add_group(0, ranked[lo:hi])
    to_owner(0).start()

    def next_round(h, carry):
        for lo, hi in zip(later, later[1:]):
            add_group(h, ranked[lo:hi])

        @pl.when(h < 2 * ny - 2)
        def _():
            to_owner(h).start()

        return carry

    lax.fori_loop(1, 2 * ny - 1, next_round, 0)

    upto = jnp.where(iota((BINS, BINS), 0) <= iota((BINS, BINS), 1), 1.0, 0.0)
    lane = iota((node_count, BINS), 1)
    low = jnp.full((), -3.0e38, f32)

    def swap(i):
        return remote(mine.at[i], acc_in.at[i], core_send.at[i], core_recv.at[i], core_mate)

    def collect(i):
        total = acc[2 * ny - 2 + i]
        for j in range(ny - 1):
            to_owner(2 * j + i).wait_recv()
            total = total + acc_y[2 * j + i]
        mine[i] = total
        swap(i).start()

    def best_of(i):
        swap(i).wait_recv()
        hist = mine[i] + acc_in[i]
        found = []
        for s in range(part):
            left = jnp.dot(hist[:, s * BINS:(s + 1) * BINS], upto, precision=lax.Precision.HIGHEST,
                           preferred_element_type=f32)
            left_grad, left_hess = left[:node_count], left[node_count:]
            total_grad, total_hess = left_grad[:, BINS - 1:], left_hess[:, BINS - 1:]
            gain = 0.5 * (left_grad * left_grad / (left_hess + l2_penalty)
                          + (total_grad - left_grad) ** 2 / (total_hess - left_hess + l2_penalty)
                          - total_grad * total_grad / (total_hess + l2_penalty))
            found.append(jnp.max(jnp.where(lane < BINS - 1, gain, low), axis=1, keepdims=True))
        return found

    collect(0)
    next_round(2 * ny - 1, 0)
    collect(1)
    best = best_of(0)
    best += best_of(1)
    half = sc // 2
    diagonal = iota((node_count, LANES), 0) == iota((node_count, LANES), 1)

    def spread(column):
        return jnp.max(jnp.where(diagonal, column, low), axis=0, keepdims=True)

    top[...] = spread(functools.reduce(jnp.maximum, best))
    for s in range(half):
        best_out[s:s + 1] = spread(jnp.where(core == 0, best[s], best[half + s]))[:, :node_count]

    others = [(dx, dy, dz) for dx in range(nx) for dy in range(ny) for dz in range(nz)][1:]
    far = {n: [min(k, n - k) for k in range(n)] for n in (nx, ny, nz)}
    others.sort(key=lambda d: -(far[nx][d[0]] + far[ny][d[1]] + far[nz][d[2]]))
    for i, (dx, dy, dz) in enumerate(others):
        remote(top, tops.at[i], top_send, top_recv,
               {"rep": lax.rem(x + dx, nx), "rows_0": lax.rem(y + dy, ny), "rows_1": lax.rem(z + dz, nz),
                "rows_2": 1 - core}).start()
    wait_for(tops, top_recv)
    node_best_out[...] = jnp.maximum(top[...], jnp.max(tops[...], axis=0))[:, :node_count]

    for copy in side_copies + [swap(0), swap(1)]:
        copy.wait_send()
    wait_for(tops, top_send)
    for k in range(1, nz):
        stats_to(k).wait_send()
        node_to(k).wait_send()
        for h in range(2 * ny):
            bins_to(h, k).wait_send()
    for h in range(2 * ny - 2):
        to_owner(h).wait_send()


def finish(nodes, best, node_best, nodes_out, best_out, node_best_out):
    nodes_out[...] = nodes[...]
    best_out[...] = best[...]
    node_best_out[...] = node_best[...]


def body(sizes, binned, gradients, hessians, parents, split_feature, split_bin, elected):
    ny, nz, nx = sizes
    rows_here, width = binned.shape
    node_count, slots_here = elected.shape
    chunks = rows_here // LANES
    sc = slots_here // (ny * nz)
    shape = (chunks, LANES)
    vmem, hbm = pl.BlockSpec(memory_space=pltpu.VMEM), pl.BlockSpec(memory_space=pl.ANY)
    dma = pltpu.SemaphoreType.DMA
    results = (
        jax.ShapeDtypeStruct((chunks, LANES), i32),
        jax.ShapeDtypeStruct((sc // 2, node_count), f32),
        jax.ShapeDtypeStruct((1, node_count), f32),
    )
    outs = pl.pallas_call(
        functools.partial(kernel, ny, nz, nx, sc),
        out_shape=tuple(pltpu.VMEM(r.shape, r.dtype) for r in results),
        in_specs=[hbm] * 7,
        out_specs=(vmem, vmem, vmem),
        scratch_shapes=[
            pltpu.SMEM(split_feature.shape, i32),
            pltpu.SMEM(split_bin.shape, i32),
            pltpu.VMEM(shape, bf16),
            pltpu.VMEM(shape, bf16),
            pltpu.VMEM(shape, i32),
            pltpu.VMEM(elected.shape, i32),
            pltpu.VMEM((rows_here, width), i32),
            pltpu.VMEM((chunks, LANES), f32),
            pltpu.VMEM((nx - 1, chunks, LANES), f32),
            pltpu.VMEM((nz, ny, sc, chunks, LANES), f32),
            pltpu.VMEM((nz, ny, sc, chunks, LANES), f32),
            pltpu.VMEM((2 * ny, nz, sc // 2, chunks, LANES), f32),
            pltpu.VMEM((nz, chunks, LANES), f32),
            pltpu.VMEM((nz, 2, chunks, LANES), f32),
            pltpu.VMEM((nz, 2 * node_count, rows_here), bf16),
            pltpu.VMEM((2 * ny, 2 * node_count, sc * BINS // 2), f32),
            pltpu.VMEM((2 * ny - 2, 2 * node_count, sc * BINS // 2), f32),
            pltpu.VMEM((2, 2 * node_count, sc * BINS // 2), f32),
            pltpu.VMEM((2, 2 * node_count, sc * BINS // 2), f32),
            pltpu.VMEM((1, LANES), f32),
            pltpu.VMEM((nx * ny * nz - 1, 1, LANES), f32),
            dma((7,)),
            dma((nx - 1,)), dma((nx - 1,)),
            dma((2 * ny, nz)), dma((2 * ny, nz)),
            dma((nz,)), dma((nz,)),
            dma((nz,)), dma((nz,)),
            dma((2 * ny - 2,)), dma((2 * ny - 2,)),
            dma((2,)), dma((2,)),
            dma, dma,
        ],
        compiler_params=pltpu.CompilerParams(collective_id=0, has_side_effects=True),
        name="level",
    )(split_feature, split_bin, gradients.reshape(shape), hessians.reshape(shape), parents.reshape(shape), elected, binned)
    nodes, best, node_best = pl.pallas_call(
        finish, out_shape=results, in_specs=[vmem] * 3, out_specs=(vmem,) * 3, name="finish"
    )(*(pltpu.with_memory_space_constraint(out, pltpu.VMEM) for out in outs))
    return nodes.reshape(rows_here), best.T[:, None, :], node_best.reshape(node_count)


def solution(mesh):
    ny, nz, nx = 4, 8, mesh.shape["rep"]
    finer = Mesh(mesh.devices.reshape(ny, nz, 2, nx), ("rows_0", "rows_1", "rows_2", "rep"))
    placed = (P(ROWS, "rep"), P(ROWS), P(ROWS), P(ROWS), P(), P(), P(None, "rep"))
    return jax.shard_map(
        functools.partial(body, (ny, nz, nx)),
        mesh=finer,
        in_specs=placed,
        out_specs=(P(ROWS), P(None, "rep", ROWS), P()),
        check_vma=False,
    )
```

```python
import functools

import jax
import jax.numpy as jnp
from jax import lax
from jax.experimental import pallas as pl
from jax.experimental.pallas import tpu as pltpu
from jax.sharding import Mesh
from jax.sharding import PartitionSpec as P

BINS = 128
LANES = 128
ROWS = ("rows_0", "rows_1", "rows_2")
MESH_IDS = pl.DeviceIdType.MESH
f32, bf16, i32, f8 = jnp.float32, jnp.bfloat16, jnp.int32, jnp.float8_e4m3fn

l2_penalty = 1.0


def iota(shape, dim, dtype=i32):
    out = lax.broadcasted_iota(i32, shape, dim)
    if dtype == bf16:
        return out.astype(f32).astype(bf16)
    return out.astype(dtype)


def remote(src, dst, send, recv, where):
    return pltpu.make_async_remote_copy(
        src_ref=src, dst_ref=dst, send_sem=send, recv_sem=recv, device_id=where, device_id_type=MESH_IDS
    )


def kernel(ny, nz, nx, sc, split_feature_hbm, split_bin_hbm, gradients_hbm, hessians_hbm, parents_hbm, elected_hbm, binned_hbm,
           nodes_out, best_out, node_best_out,
           split_feature, split_bin, gradients, hessians, parents, elected, binned, side, side_in, left_box, outbox, zbox, node_box, stats_box, weights, acc, acc_y, mine, acc_in,
           top, tops,
           load_sems, side_send, side_recv, z_send, z_recv, node_send, node_recv, stats_send, stats_recv,
           y_send, y_recv, core_send, core_recv, top_send, top_recv):
    y, z = lax.axis_index("rows_0"), lax.axis_index("rows_1")
    core, x = lax.axis_index("rows_2"), lax.axis_index("rep")
    parent_count = split_feature.shape[0]
    node_count = elected.shape[0]
    width = binned.shape[1]
    chunks = parents.shape[0]

    def at_x(d):
        return {"rep": lax.rem(x + d, nx)}

    def at_y(d):
        return {"rows_0": lax.rem(y + d, ny)}

    def at_z(d):
        return {"rows_1": lax.rem(z + d, nz), "rows_2": 1 - core}

    core_mate = {"rows_2": 1 - core}
    beside = [at_x(d) for d in range(1, nx)] + [at_y(d) for d in range(1, ny)] + [core_mate] + [at_z(d) for d in range(1, nz)]
    ranked = [4, 3, 5, 2, 6, 1, 7] if nz == 8 else list(range(1, nz))
    barrier = pltpu.get_barrier_semaphore()
    for peer in beside:
        pl.semaphore_signal(barrier, inc=1, device_id=peer, device_id_type=MESH_IDS)

    pairs = ((binned_hbm, binned), (parents_hbm, parents), (split_feature_hbm, split_feature), (split_bin_hbm, split_bin),
             (gradients_hbm, gradients), (hessians_hbm, hessians), (elected_hbm, elected))
    loads = [pltpu.make_async_copy(src, dst, load_sems.at[i]) for i, (src, dst) in enumerate(pairs)]
    for load in loads:
        load.start()

    for load in loads[1:]:
        load.wait()
    stats_box[0, 0] = gradients[...].astype(f32)
    stats_box[0, 1] = hessians[...].astype(f32)
    parent = parents[...].astype(f32)
    parent_rows = iota((parent_count, LANES), 0)
    want = jnp.zeros((parent_count, width), i32)
    bound = jnp.zeros((parent_count, LANES), i32)
    for p in range(parent_count):
        want = jnp.where(iota((parent_count, width), 0) == p, split_feature[p] - x * width, want)
        bound = jnp.where(parent_rows == p, split_bin[p], bound)
    pick = jnp.where(iota((parent_count, width), 1) == want, jnp.ones((), f32), jnp.zeros((), f32)).astype(bf16)
    owned = (want[:, :LANES] >= 0) & (want[:, :LANES] < width)
    loads[0].wait()
    values = lax.dot_general(pick, binned[...].astype(f32).astype(bf16), (((1,), (1,)), ((), ())),
                             preferred_element_type=f32)
    bound = bound.astype(f32)
    for c in range(chunks):
        hit = (parent_rows.astype(f32) == parent[c:c + 1]) & owned & (values[:, c * LANES:(c + 1) * LANES] > bound)
        side[c:c + 1, :] = jnp.max(jnp.where(hit, 1.0, 0.0), axis=0, keepdims=True)

    pl.semaphore_wait(barrier, len(beside))
    side_copies = []
    for d in range(1, nx):
        copy = remote(side, side_in.at[d - 1], side_send.at[d - 1], side_recv.at[d - 1], at_x(d))
        copy.start()
        side_copies.append(copy)
    def stats_to(k):
        return remote(stats_box.at[0], stats_box.at[k], stats_send.at[k], stats_recv.at[k], at_z(k))

    def node_to(k):
        return remote(node_box.at[0], node_box.at[k], node_send.at[k], node_recv.at[k], at_z(k))

    part = sc // 2

    def bins_to(h, k):
        there, lo = lax.rem(y + 1 + h // 2, ny), h % 2 * part
        return remote(outbox.at[lax.rem(z + k, nz), there, pl.ds(lo, part)], zbox.at[h, k],
                      z_send.at[h, k], z_recv.at[h, k], at_z(k))

    def send_stats():
        for k in ranked:
            stats_to(k).start()

    def send_rows():
        for k in ranked:
            node_to(k).start()
        for h in range(2 * ny):
            for k in ranked:
                bins_to(h, k).start()

    send_stats()

    chosen = elected[...].astype(f32).astype(bf16)
    node_rows = iota((node_count, LANES), 0).astype(f32)
    for c in range(chunks):
        rows = slice(c * LANES, (c + 1) * LANES)
        packed = binned[rows, :LANES]
        for b in range(1, width // LANES):
            packed = packed + (binned[rows, b * LANES:(b + 1) * LANES] << (8 * b))
        for way, box in ((0, left_box), (1, outbox)):
            hot = jnp.where(node_rows == 2.0 * parent[c:c + 1] + way, 1.0, 0.0).astype(bf16)
            index = lax.dot_general(hot, chosen, (((0,), (0,)), ((), ())), preferred_element_type=f32).astype(i32)
            found = jnp.take_along_axis(packed, index & (LANES - 1), axis=1, mode="promise_in_bounds")
            found = (found >> ((index >> 7) << 3)) & (BINS - 1)
            turned = found.astype(f32).T
            for yy in range(ny):
                for zz in range(nz):
                    first = (yy * nz + zz) * sc
                    box[zz, yy, :, c, :] = turned[first:first + sc]

    for copy in side_copies:
        copy.wait_recv()
    went = side[...]
    for d in range(1, nx):
        went = went + side_in[d - 1]
    node = 2.0 * parent + went
    nodes_out[...] = node.astype(i32)
    node_box[0] = node
    right = (went > 0.0)[None]
    for yy in range(ny):
        for zz in range(nz):
            outbox[zz, yy] = jnp.where(right, outbox[zz, yy], left_box[zz, yy])
    send_rows()

    def weigh(d):
        node_of = iota((node_count, LANES), 0, bf16)
        zero = jnp.zeros((), bf16)
        for c in range(chunks):
            here = node_of == node_box[d, c:c + 1, :].astype(bf16)
            at = slice(c * LANES, (c + 1) * LANES)
            weights[d, :node_count, at] = jnp.where(here, stats_box[d, 0, c:c + 1, :].astype(bf16), zero)
            weights[d, node_count:, at] = jnp.where(here, stats_box[d, 1, c:c + 1, :].astype(bf16), zero)

    def counted(box, d):
        bin_rows = iota((BINS, LANES), 0, bf16)
        one, zero = jnp.ones((), bf16), jnp.zeros((), bf16)
        hots = []
        for s in range(part):
            row = [box[s, c:c + 1, :].astype(bf16) for c in range(chunks)]
            hots.append(jnp.concatenate([jnp.where(bin_rows == r, one, zero) for r in row], axis=1))
        return lax.dot_general(weights[d], jnp.concatenate(hots, axis=0).astype(f8), (((1,), (1,)), ((), ())),
                               preferred_element_type=f32)

    def wait_for(ref, sem):
        pltpu.make_async_copy(ref, ref, sem).wait()

    weigh(0)

    def own(h, carry):
        acc[h] = counted(outbox.at[z, lax.rem(y + 1 + h // 2, ny), pl.ds(h % 2 * part, part)], 0)
        return carry

    lax.fori_loop(0, 2 * ny, own, 0)
    def to_owner(h):
        return remote(acc.at[h], acc_y.at[h], y_send.at[h], y_recv.at[h], at_y(1 + h // 2))

    def add_group(h, group):
        for d in group:
            wait_for(zbox.at[h, d], z_recv.at[h, d])
        acc[h] += functools.reduce(jnp.add, [counted(zbox.at[h, d], d) for d in group])

    cuts, later = ([0, 2, 4, 6, 7], [0, 7]) if nz == 8 else ([0, nz - 1],) * 2
    for lo, hi in zip(cuts, cuts[1:]):
        for d in ranked[lo:hi]:
            wait_for(stats_box.at[d], stats_recv.at[d])
            wait_for(node_box.at[d], node_recv.at[d])
            weigh(d)
        add_group(0, ranked[lo:hi])
    to_owner(0).start()

    def next_round(h, carry):
        for lo, hi in zip(later, later[1:]):
            add_group(h, ranked[lo:hi])

        @pl.when(h < 2 * ny - 2)
        def _():
            to_owner(h).start()

        return carry

    lax.fori_loop(1, 2 * ny - 1, next_round, 0)

    upto = jnp.where(iota((BINS, BINS), 0) <= iota((BINS, BINS), 1), 1.0, 0.0)
    lane = iota((node_count, BINS), 1)
    low = jnp.full((), -3.0e38, f32)

    def swap(i):
        return remote(mine.at[i], acc_in.at[i], core_send.at[i], core_recv.at[i], core_mate)

    def collect(i):
        total = acc[2 * ny - 2 + i]
        for j in range(ny - 1):
            to_owner(2 * j + i).wait_recv()
            total = total + acc_y[2 * j + i]
        mine[i] = total
        swap(i).start()

    def best_of(i):
        swap(i).wait_recv()
        hist = mine[i] + acc_in[i]
        found = []
        for s in range(part):
            left = jnp.dot(hist[:, s * BINS:(s + 1) * BINS], upto, precision=lax.Precision.HIGHEST,
                           preferred_element_type=f32)
            left_grad, left_hess = left[:node_count], left[node_count:]
            total_grad, total_hess = left_grad[:, BINS - 1:], left_hess[:, BINS - 1:]
            gain = 0.5 * (left_grad * left_grad / (left_hess + l2_penalty)
                          + (total_grad - left_grad) ** 2 / (total_hess - left_hess + l2_penalty)
                          - total_grad * total_grad / (total_hess + l2_penalty))
            found.append(jnp.max(jnp.where(lane < BINS - 1, gain, low), axis=1, keepdims=True))
        return found

    next_round(2 * ny - 1, 0)
    collect(0)
    collect(1)
    best = best_of(0)
    best += best_of(1)
    half = sc // 2
    diagonal = iota((node_count, LANES), 0) == iota((node_count, LANES), 1)

    def spread(column):
        return jnp.max(jnp.where(diagonal, column, low), axis=0, keepdims=True)

    top[...] = spread(functools.reduce(jnp.maximum, best))
    for s in range(half):
        best_out[s:s + 1] = spread(jnp.where(core == 0, best[s], best[half + s]))[:, :node_count]

    others = [(dx, dy, dz) for dx in range(nx) for dy in range(ny) for dz in range(nz)][1:]
    far = {n: [min(k, n - k) for k in range(n)] for n in (nx, ny, nz)}
    others.sort(key=lambda d: -(far[nx][d[0]] + far[ny][d[1]] + far[nz][d[2]]))
    for i, (dx, dy, dz) in enumerate(others):
        remote(top, tops.at[i], top_send, top_recv,
               {"rep": lax.rem(x + dx, nx), "rows_0": lax.rem(y + dy, ny), "rows_1": lax.rem(z + dz, nz),
                "rows_2": 1 - core}).start()
    wait_for(tops, top_recv)
    node_best_out[...] = jnp.maximum(top[...], jnp.max(tops[...], axis=0))[:, :node_count]

    for copy in side_copies + [swap(0), swap(1)]:
        copy.wait_send()
    wait_for(tops, top_send)
    for k in range(1, nz):
        stats_to(k).wait_send()
        node_to(k).wait_send()
        for h in range(2 * ny):
            bins_to(h, k).wait_send()
    for h in range(2 * ny - 2):
        to_owner(h).wait_send()


def finish(nodes, best, node_best, nodes_out, best_out, node_best_out):
    nodes_out[...] = nodes[...]
    best_out[...] = best[...]
    node_best_out[...] = node_best[...]


def body(sizes, binned, gradients, hessians, parents, split_feature, split_bin, elected):
    ny, nz, nx = sizes
    rows_here, width = binned.shape
    node_count, slots_here = elected.shape
    chunks = rows_here // LANES
    sc = slots_here // (ny * nz)
    shape = (chunks, LANES)
    vmem, hbm = pl.BlockSpec(memory_space=pltpu.VMEM), pl.BlockSpec(memory_space=pl.ANY)
    dma = pltpu.SemaphoreType.DMA
    results = (
        jax.ShapeDtypeStruct((chunks, LANES), i32),
        jax.ShapeDtypeStruct((sc // 2, node_count), f32),
        jax.ShapeDtypeStruct((1, node_count), f32),
    )
    outs = pl.pallas_call(
        functools.partial(kernel, ny, nz, nx, sc),
        out_shape=tuple(pltpu.VMEM(r.shape, r.dtype) for r in results),
        in_specs=[hbm] * 7,
        out_specs=(vmem, vmem, vmem),
        scratch_shapes=[
            pltpu.SMEM(split_feature.shape, i32),
            pltpu.SMEM(split_bin.shape, i32),
            pltpu.VMEM(shape, bf16),
            pltpu.VMEM(shape, bf16),
            pltpu.VMEM(shape, i32),
            pltpu.VMEM(elected.shape, i32),
            pltpu.VMEM((rows_here, width), i32),
            pltpu.VMEM((chunks, LANES), f32),
            pltpu.VMEM((nx - 1, chunks, LANES), f32),
            pltpu.VMEM((nz, ny, sc, chunks, LANES), f32),
            pltpu.VMEM((nz, ny, sc, chunks, LANES), f32),
            pltpu.VMEM((2 * ny, nz, sc // 2, chunks, LANES), f32),
            pltpu.VMEM((nz, chunks, LANES), f32),
            pltpu.VMEM((nz, 2, chunks, LANES), f32),
            pltpu.VMEM((nz, 2 * node_count, rows_here), bf16),
            pltpu.VMEM((2 * ny, 2 * node_count, sc * BINS // 2), f32),
            pltpu.VMEM((2 * ny - 2, 2 * node_count, sc * BINS // 2), f32),
            pltpu.VMEM((2, 2 * node_count, sc * BINS // 2), f32),
            pltpu.VMEM((2, 2 * node_count, sc * BINS // 2), f32),
            pltpu.VMEM((1, LANES), f32),
            pltpu.VMEM((nx * ny * nz - 1, 1, LANES), f32),
            dma((7,)),
            dma((nx - 1,)), dma((nx - 1,)),
            dma((2 * ny, nz)), dma((2 * ny, nz)),
            dma((nz,)), dma((nz,)),
            dma((nz,)), dma((nz,)),
            dma((2 * ny - 2,)), dma((2 * ny - 2,)),
            dma((2,)), dma((2,)),
            dma, dma,
        ],
        compiler_params=pltpu.CompilerParams(collective_id=0, has_side_effects=True),
        name="level",
    )(split_feature, split_bin, gradients.reshape(shape), hessians.reshape(shape), parents.reshape(shape), elected, binned)
    nodes, best, node_best = pl.pallas_call(
        finish, out_shape=results, in_specs=[vmem] * 3, out_specs=(vmem,) * 3, name="finish"
    )(*(pltpu.with_memory_space_constraint(out, pltpu.VMEM) for out in outs))
    return nodes.reshape(rows_here), best.T[:, None, :], node_best.reshape(node_count)


def solution(mesh):
    ny, nz, nx = 4, 8, mesh.shape["rep"]
    finer = Mesh(mesh.devices.reshape(ny, nz, 2, nx), ("rows_0", "rows_1", "rows_2", "rep"))
    placed = (P(ROWS, "rep"), P(ROWS), P(ROWS), P(ROWS), P(), P(), P(None, "rep"))
    return jax.shard_map(
        functools.partial(body, (ny, nz, nx)),
        mesh=finer,
        in_specs=placed,
        out_specs=(P(ROWS), P(None, "rep", ROWS), P()),
        check_vma=False,
    )
```
